32 devices in a mesh: seq: 4 (over y, x), fsdp: 8 (over z, core).
Axes of the slice: x: 2, y: 2, z: 4, core: 2. Of those that a mesh axis runs over, the one named last changes fastest.
Arguments:
- hidden_in: bfloat16 [8, 1024, 2048], P('fsdp', 'seq'), may hold values from -6 to 6
- cotangent: bfloat16 [8, 1024, 2048], P('fsdp', 'seq'), may hold values from -6 to 6
- block_table: int32 [4, 2], replicated, may hold values from 0 to 7, as said below
- first_gain: bfloat16 [2048], P('fsdp'), may hold values from 0.5 to 1.5
- first_bias: bfloat16 [2048], P('fsdp'), may hold values from -3 to 3
- qkv_weight: bfloat16 [2048, 6144], P('fsdp'), may hold values from -0.125 to 0.125
- qkv_bias: bfloat16 [6144], P('fsdp')
- out_weight: bfloat16 [2048, 2048], P('fsdp'), may hold values from -2 to 2
- second_gain: bfloat16 [2048], P('fsdp'), may hold values from 0.5 to 1.5
- second_bias: bfloat16 [2048], P('fsdp'), may hold values from -3 to 3
- gate_weight: bfloat16 [2048, 5632], P('fsdp'), may hold values from -0.125 to 0.125
- up_weight: bfloat16 [2048, 5632], P('fsdp'), may hold values from -0.125 to 0.125
- down_weight: bfloat16 [5632, 2048], P('fsdp'), may hold values from -0.078125 to 0.078125
Outputs:
- block_out: bfloat16 [8, 1024, 2048], P('fsdp', 'seq')
- input_grad: bfloat16 [8, 1024, 2048], P('fsdp', 'seq')
- first_gain_grad: float32 [2048], P('fsdp')
- first_bias_grad: float32 [2048], P('fsdp')
- qkv_weight_grad: float32 [2048, 6144], P('fsdp')
- qkv_bias_grad: float32 [6144], P('fsdp')
- out_weight_grad: float32 [2048, 2048], P('fsdp')
- second_gain_grad: float32 [2048], P('fsdp')
- second_bias_grad: float32 [2048], P('fsdp')
- gate_weight_grad: float32 [2048, 5632], P('fsdp')
- up_weight_grad: float32 [2048, 5632], P('fsdp')
- down_weight_grad: float32 [5632, 2048], P('fsdp')
The draws below stay inside these ranges and needn't reach their ends.
Inputs may be any that keep to these rules, and one draw needn't show every extreme that they name: `block_table`: row i holds a pair b and 7 - b, in either order; every block number appears once in the table; the same table holds for all sequences.
All inputs are finite; a program needn't handle non-finite values.
Results may differ from the reference program's by a relative error of at most 0.028.
The reference program's roundings to bfloat16 on the way count: a program that leaves them out, or rounds other values in their place, can miss the bound.
Values may be sent and summed in bfloat16 or wider, within the bound.
A program may use at most 448 MiB of HBM per device.

```python
import jax
import jax.numpy as jnp
from jax import lax

D = 2048
HEADS = 32
HD = 64
FF = 5632
BLK = 128
SEQS = 8
L = 1024
N_SEQ = 4


def draw_block_table(key, part):
    perm_key = jax.random.fold_in(key, 31)
    flip_key = jax.random.fold_in(key, 47)
    chosen = jax.random.permutation(perm_key, N_SEQ).astype(jnp.int32)
    flips = jax.random.randint(flip_key, (N_SEQ,), 0, 2).astype(jnp.int32)
    mirror = 2 * N_SEQ - 1 - chosen
    first = jnp.where(flips == 1, mirror, chosen)
    second = jnp.where(flips == 1, chosen, mirror)
    return jnp.stack([first, second], axis=1).astype(jnp.int32)


def draw_qkv_bias(key, part):
    base = jax.random.normal(key, (3 * D,), jnp.float32) * 0.5
    return base.astype(jnp.bfloat16)


def levels(key, shape, pieces, smallest, high):
    def one(position, blocks):
        heights = jax.random.uniform(jax.random.fold_in(jax.random.fold_in(key, 6), position), (blocks,), jnp.float32, smallest / len(pieces), high / len(pieces))
        return jnp.repeat(jnp.exp(heights), shape[position] // blocks).reshape((-1,) + (1,) * (len(shape) - position - 1))

    factor_of = one(*pieces[0])
    for cut in pieces[1:]:
        factor_of = factor_of * one(*cut)
    return factor_of


def bell_draw(own_key, dims, scale, reach, cuts=(), kind=jnp.bfloat16):
    values = jax.random.normal(own_key, dims, jnp.float32) * scale
    if len(cuts) > 0:
        values = levels(own_key, dims, cuts, -0.22, 0.18) * values
    return jnp.clip(values, min=-reach, max=reach).astype(kind)


def setup_inputs(seed: int = 0) -> dict:
    streams_of = jax.random.split(jax.random.key(seed), 14)
    return {
        "hidden_in": bell_draw(streams_of[0], (SEQS, L, D), 1.0, 6.0, ((0, 8), (1, 4))),
        "cotangent": bell_draw(streams_of[1], (SEQS, L, D), 1.0, 6.0, ((0, 8), (1, 4))),
        "block_table": draw_block_table(jax.random.fold_in(streams_of[13], 71), 0),
        "first_gain": jnp.clip(1.0 + 0.1 * jax.random.normal(streams_of[3], (D,), jnp.float32), 0.5, 1.5).astype(jnp.bfloat16),
        "first_bias": bell_draw(streams_of[4], (D,), 0.5, 3.0, ((0, 8),)),
        "qkv_weight": bell_draw(streams_of[5], (D, 3 * D), D ** -0.5, 0.125, ((0, 8),)),
        "qkv_bias": draw_qkv_bias(jax.random.fold_in(streams_of[13], 71), 0),
        "out_weight": bell_draw(streams_of[7], (D, D), (max(D // 256, 1)) ** -0.5, 2.0, ((0, 8),)),
        "second_gain": jnp.clip(1.0 + 0.1 * jax.random.normal(streams_of[8], (D,), jnp.float32), 0.5, 1.5).astype(jnp.bfloat16),
        "second_bias": bell_draw(streams_of[9], (D,), 0.5, 3.0, ((0, 8),)),
        "gate_weight": bell_draw(streams_of[10], (D, FF), D ** -0.5, 0.125, ((0, 8),)),
        "up_weight": bell_draw(streams_of[11], (D, FF), D ** -0.5, 0.125, ((0, 8),)),
        "down_weight": bell_draw(streams_of[12], (FF, D), FF ** -0.5, 0.078125, ((0, 8),)),
    }


EPS = 1e-05
ROPE_BASE = 10000.0
NEG = -1e+30
HIGH = lax.Precision.HIGHEST

@jax.custom_vjp
def low(v):
    return lax.optimization_barrier(v.astype(jnp.bfloat16)).astype(jnp.float32)

@jax.custom_vjp
def low_back(v):
    return v

def low_keep(v):
    return (low(v), None)

def low_pass(kept, grad):
    return (grad,)

def back_keep(v):
    return (v, None)

def back_low(kept, grad):
    return (low(grad),)
low.defvjp(low_keep, low_pass)
low_back.defvjp(back_keep, back_low)

def layer_norm(values, gain, shift):
    centred = values - lax.optimization_barrier(jnp.mean(values, axis=-1, keepdims=True))
    inverse = lax.rsqrt(lax.optimization_barrier(jnp.mean(centred * centred, axis=-1, keepdims=True)) + EPS)
    return centred * inverse * gain + shift

def rotate(tensor, places, direction):
    head_dim = tensor.shape[-1]
    rotated = head_dim // 4
    half = rotated // 2
    freq = ROPE_BASE ** (-(jnp.arange(half, dtype=jnp.float32) * 2.0) / rotated)
    angle = places.astype(jnp.float32)[:, None] * freq[None, :]
    cosine = jnp.cos(angle)[:, None, :]
    sine = direction * jnp.sin(angle)[:, None, :]
    first = tensor[..., :half]
    second = tensor[..., half:rotated]
    return jnp.concatenate([first * cosine - second * sine, second * cosine + first * sine, tensor[..., rotated:]], axis=-1)

def reference(hidden_in, cotangent, block_table, first_gain, first_bias, qkv_weight, qkv_bias, out_weight, second_gain, second_bias, gate_weight, up_weight, down_weight):
    slot_blocks = block_table.reshape(-1).astype(jnp.int32)
    block_slots = jnp.argsort(slot_blocks).astype(jnp.int32)
    blocks = 2 * N_SEQ

    def to_sequence(array):
        return array.reshape(SEQS, blocks, BLK, D)[:, block_slots].reshape(SEQS, L, D)

    def to_storage(array):
        return array.reshape(SEQS, blocks, BLK, D)[:, slot_blocks].reshape(SEQS, L, D)
    params = tuple((item.astype(jnp.float32) for item in (first_gain, first_bias, qkv_weight, qkv_bias, out_weight, second_gain, second_bias, gate_weight, up_weight, down_weight)))
    places = jnp.arange(L, dtype=jnp.int32)
    causal = places[None, :] <= places[:, None]
    scale = HD ** (-0.5)

    def one_head(triple):
        query_head, key_head, value_head = triple
        scores = low_back(jnp.dot(query_head, key_head.T, precision=HIGH) * scale)
        scores = jnp.where(causal, scores, NEG)
        peak = lax.optimization_barrier(jnp.max(scores, axis=-1, keepdims=True))
        log_total = peak + jnp.log(lax.optimization_barrier(jnp.sum(jnp.exp(scores - peak), axis=-1, keepdims=True)))
        weights = low(jnp.exp(scores - log_total))
        return jnp.dot(weights, value_head, precision=HIGH)

    def forward(inputs, gain_one, bias_one, w_qkv, b_qkv, w_out, gain_two, bias_two, w_gate, w_up, w_down):
        normed_one = low(layer_norm(inputs, gain_one, bias_one))
        projected = low_back(jnp.dot(normed_one, w_qkv, precision=HIGH) + b_qkv)
        query = low(rotate(projected[:, :D].reshape(L, HEADS, HD), places, 1.0))
        keys = low(rotate(projected[:, D:2 * D].reshape(L, HEADS, HD), places, 1.0))
        values = low(projected[:, 2 * D:].reshape(L, HEADS, HD))
        head_out = lax.map(jax.checkpoint(one_head), (query.transpose(1, 0, 2), keys.transpose(1, 0, 2), values.transpose(1, 0, 2)))
        mixed = low_back(low(head_out.transpose(1, 0, 2).reshape(L, D)))
        residual = inputs + low_back(jnp.dot(mixed, w_out, precision=HIGH))
        normed_two = low(layer_norm(residual, gain_two, bias_two))
        gate = low_back(jnp.dot(normed_two, w_gate, precision=HIGH))
        upward = low_back(jnp.dot(normed_two, w_up, precision=HIGH))
        activated = low(jax.nn.silu(gate) * upward)
        return residual + low_back(jnp.dot(activated, w_down, precision=HIGH))

    def one_sequence(totals, pair):
        inputs, d_out = pair
        output, pull = jax.vjp(forward, inputs, *params)
        grads = pull(d_out)
        return (tuple((total + grad for total, grad in zip(totals, grads[1:]))), (output, grads[0]))
    start_totals = tuple((jnp.zeros_like(item) for item in params))
    totals, (outputs, d_inputs) = lax.scan(one_sequence, start_totals, (to_sequence(hidden_in.astype(jnp.float32)), to_sequence(cotangent.astype(jnp.float32))))
    return (to_storage(outputs).astype(jnp.bfloat16), to_storage(d_inputs).astype(jnp.bfloat16), totals[0], totals[1], totals[2], totals[3], totals[4], totals[5], totals[6], totals[7], totals[8], totals[9])
```

```python
import functools

import jax
import jax.numpy as jnp
from jax import lax
from jax.experimental import pallas as pl
from jax.experimental.pallas import tpu as pltpu
from jax.sharding import PartitionSpec as P

HEADS = 32
HD = 64
ROT = HD // 4
HALF = ROT // 2
EPS = 1e-05
ROPE_BASE = 10000.0
NEG = -1e30
SCALE = float(HD) ** -0.5
f32 = jnp.float32
bf16 = jnp.bfloat16


def normalize(values):
    centred = values - jnp.mean(values, axis=-1, keepdims=True)
    inverse = lax.rsqrt(jnp.mean(centred * centred, axis=-1, keepdims=True) + EPS)
    return (centred * inverse, inverse)


def norm_back(d_normed, normed, inverse, gain):
    scaled = d_normed * gain
    return inverse * (
        scaled
        - jnp.mean(scaled, axis=-1, keepdims=True)
        - normed * jnp.mean(scaled * normed, axis=-1, keepdims=True)
    )


def swap(value, mask, n):
    return lax.ppermute(value, "seq", [(i, i ^ mask) for i in range(n)])


def cuts(count, parts):
    edges = [(count * i // parts + 8) // 16 * 16 for i in range(parts)] + [count]
    return [(a, b) for a, b in zip(edges, edges[1:]) if b > a]


def gather_seq(value, n):
    bits = n.bit_length() - 1
    streams = []
    for index, (first, last) in enumerate(cuts(value.shape[0], bits)):
        have = {0: value[first:last]}
        for step in range(bits):
            mask = 1 << ((index + step) % bits)
            have.update({key ^ mask: swap(item, mask, n) for key, item in have.items()})
        streams.append(have)
    return [jnp.concatenate([have[j] for have in streams], axis=0) for j in range(n)]


def scatter_seq(pieces, n):
    bits = n.bit_length() - 1
    streams = []
    for index, (first, last) in enumerate(cuts(pieces[0].shape[0], bits)):
        have = {j: pieces[j][first:last] for j in range(n)}
        for step in range(bits):
            mask = 1 << ((index + bits - 1 - step) % bits)
            got = {
                key ^ mask: swap(item.astype(bf16), mask, n)
                for key, item in have.items()
                if key & mask
            }
            have = {
                key: item + got[key].astype(f32)
                for key, item in have.items()
                if not key & mask
            }
        streams.append(have[0])
    return jnp.concatenate(streams, axis=0)


def exchange_seq(pieces, n):
    return [pieces[0]] + [swap(pieces[j], j, n) for j in range(1, n)]


def choose(index, options):
    out = options[0]
    for i, option in enumerate(options[1:], 1):
        out = jnp.where(index == i, option, out)
    return out


def turn(tensor, cosine, left, right, sign):
    back = pltpu.roll(tensor, 2 * HD - HALF, 1)
    ahead = pltpu.roll(tensor, HALF, 1)
    return tensor * cosine + sign * (back * left + ahead * right)


def attend_kernel(slot_ref, q_ref, k_ref, v_ref, cos_ref, left_ref, right_ref,
                  o_ref, lse_ref, qo_ref, ko_ref, vo_ref, tile):
    tokens = q_ref.shape[0]
    slots = slot_ref.shape[0]
    blk = tokens // slots
    for p in range(slots):
        rows = pl.ds(pl.multiple_of(slot_ref[p] * blk, blk), blk)
        own = pl.ds(p * blk, blk)
        cosine, left, right = cos_ref[own, :], left_ref[own, :], right_ref[own, :]
        qo_ref[own, :] = turn(q_ref[rows, :], cosine, left, right, 1.0).astype(bf16)
        ko_ref[own, :] = turn(k_ref[rows, :], cosine, left, right, 1.0).astype(bf16)
        vo_ref[own, :] = v_ref[rows, :].astype(bf16)
    mask = lax.broadcasted_iota(jnp.int32, (tile, tile), 1) <= lax.broadcasted_iota(
        jnp.int32, (tile, tile), 0
    )
    for t in range(tokens // tile):
        own = pl.ds(t * tile, tile)
        outs, stats = [], []
        for h in range(2):
            lanes = pl.ds(h * HD, HD)
            query = qo_ref[own, lanes]
            end = (t + 1) * tile
            scores = lax.dot_general(
                query, ko_ref[pl.ds(0, end), lanes], (((1,), (1,)), ((), ())),
                preferred_element_type=f32) * SCALE
            diag = jnp.where(mask, scores[:, t * tile :], NEG)
            scores = jnp.concatenate([scores[:, : t * tile], diag], axis=1) if t else diag
            peak = jnp.max(scores, axis=1, keepdims=True)
            weights = jnp.exp(scores - peak)
            total = jnp.sum(weights, axis=1, keepdims=True)
            weights = (weights * (1.0 / total)).astype(bf16)
            outs.append(jnp.dot(weights, vo_ref[pl.ds(0, end), lanes],
                                preferred_element_type=f32))
            stats.append(peak + jnp.log(total))
        out = jnp.concatenate(outs, axis=1).astype(bf16)
        lse_ref[0, own, :] = jnp.concatenate(stats, axis=1)
        for part in range(tile // blk):
            rows = pl.ds(pl.multiple_of(slot_ref[t * (tile // blk) + part] * blk, blk), blk)
            o_ref[rows, :] = out[part * blk : (part + 1) * blk]


def attend(slot, projected, tables, tile=256):
    tokens, width = projected.shape
    width //= 3
    groups = width // (2 * HD)
    lanes = 2 * HD
    col = lambda base: pl.BlockSpec((tokens, lanes), lambda i, s: (0, base + i))
    table = pl.BlockSpec((tokens, lanes), lambda i, s: (0, 0))
    return pl.pallas_call(
        functools.partial(attend_kernel, tile=tile),
        grid_spec=pltpu.PrefetchScalarGridSpec(
            num_scalar_prefetch=1,
            grid=(groups,),
            in_specs=[col(0), col(groups), col(2 * groups), table, table, table],
            out_specs=[col(0), pl.BlockSpec((1, tokens, 2), lambda i, s: (i, 0, 0)),
                       col(0), col(0), col(0)],
        ),
        out_shape=[
            jax.ShapeDtypeStruct((tokens, width), bf16),
            jax.ShapeDtypeStruct((groups, tokens, 2), f32),
            jax.ShapeDtypeStruct((tokens, width), bf16),
            jax.ShapeDtypeStruct((tokens, width), bf16),
            jax.ShapeDtypeStruct((tokens, width), bf16),
        ],
        cost_estimate=pl.CostEstimate(
            flops=4 * tokens * tokens * width, bytes_accessed=24 * tokens * width,
            transcendentals=tokens * tokens * 2 * groups),
        name="attend",
    )(slot, projected, projected, projected, *tables)


def attend_back_kernel(slot_ref, q_ref, k_ref, v_ref, d_ref, lse_ref,
                       cos_ref, left_ref, right_ref, g_ref,
                       d_pos, dq_acc, dk_acc, dv_acc, tile):
    tokens = q_ref.shape[0]
    slots = slot_ref.shape[0]
    blk = tokens // slots
    width = g_ref.shape[1] // 3
    group = pl.program_id(0)
    for p in range(slots):
        rows = pl.ds(pl.multiple_of(slot_ref[p] * blk, blk), blk)
        d_pos[pl.ds(p * blk, blk), :] = d_ref[rows, :]
    dk_acc[...] = jnp.zeros_like(dk_acc)
    dv_acc[...] = jnp.zeros_like(dv_acc)
    mask = lax.broadcasted_iota(jnp.int32, (tile, tile), 0) <= lax.broadcasted_iota(
        jnp.int32, (tile, tile), 1
    )
    for t in range(tokens // tile):
        own = pl.ds(t * tile, tile)
        past = pl.ds(0, (t + 1) * tile)
        grads = []
        keys_grad, values_grad = [], []
        for h in range(2):
            lanes = pl.ds(h * HD, HD)
            query, keys = q_ref[own, lanes], k_ref[past, lanes]
            d_out = d_pos[own, lanes]
            scores = lax.dot_general(keys, query, (((1,), (1,)), ((), ())),
                                     preferred_element_type=f32) * SCALE
            diag = jnp.where(mask, scores[t * tile :], NEG)
            scores = jnp.concatenate([scores[: t * tile], diag], axis=0) if t else diag
            probs = jnp.exp(scores - lse_ref[0, pl.ds(h, 1), own])
            d_probs = lax.dot_general(v_ref[past, lanes], d_out, (((1,), (1,)), ((), ())),
                                      preferred_element_type=f32)
            delta = jnp.sum(d_probs * probs, axis=0, keepdims=True)
            d_scores = (probs * (d_probs - delta)).astype(bf16)
            values_grad.append(jnp.dot(probs.astype(bf16), d_out, preferred_element_type=f32))
            keys_grad.append(jnp.dot(d_scores, query, preferred_element_type=f32))
            grads.append(lax.dot_general(d_scores, keys, (((0,), (0,)), ((), ())),
                                         preferred_element_type=f32))
        dk_acc[past, :] += jnp.concatenate(keys_grad, axis=1)
        dv_acc[past, :] += jnp.concatenate(values_grad, axis=1)
        dq_acc[own, :] = jnp.concatenate(grads, axis=1)
    lanes = 2 * HD
    for p in range(slots):
        rows = pl.ds(pl.multiple_of(slot_ref[p] * blk, blk), blk)
        own = pl.ds(p * blk, blk)
        cosine, left, right = cos_ref[own, :], left_ref[own, :], right_ref[own, :]
        first = pl.multiple_of(group * lanes, lanes)
        g_ref[rows, pl.ds(first, lanes)] = turn(
            dq_acc[own, :] * SCALE, cosine, left, right, -1.0).astype(bf16)
        g_ref[rows, pl.ds(width + first, lanes)] = turn(
            dk_acc[own, :] * SCALE, cosine, left, right, -1.0).astype(bf16)
        g_ref[rows, pl.ds(2 * width + first, lanes)] = dv_acc[own, :].astype(bf16)


def attend_back(slot, query, key, value, d_mixed, lse, tables, tile=256):
    tokens, width = query.shape
    groups = width // (2 * HD)
    lanes = 2 * HD
    col = pl.BlockSpec((tokens, lanes), lambda i, s: (0, i))
    table = pl.BlockSpec((tokens, lanes), lambda i, s: (0, 0))
    return pl.pallas_call(
        functools.partial(attend_back_kernel, tile=tile),
        grid_spec=pltpu.PrefetchScalarGridSpec(
            num_scalar_prefetch=1,
            grid=(groups,),
            in_specs=[col, col, col, col,
                      pl.BlockSpec((1, 2, tokens), lambda i, s: (i, 0, 0)),
                      table, table, table],
            out_specs=pl.BlockSpec((tokens, 3 * width), lambda i, s: (0, 0)),
            scratch_shapes=[pltpu.VMEM((tokens, lanes), bf16)]
            + [pltpu.VMEM((tokens, lanes), f32)] * 3,
        ),
        out_shape=jax.ShapeDtypeStruct((tokens, 3 * width), bf16),
        cost_estimate=pl.CostEstimate(
            flops=10 * tokens * tokens * width, bytes_accessed=16 * tokens * width,
            transcendentals=tokens * tokens * 2 * groups),
        name="attend_back",
    )(slot, query, key, value, d_mixed, lse, *tables)


def unpick_kernel(s_ref, in_ref, gate_ref, up_ref, shards):
    n, _, units = in_ref.shape
    units //= 2
    piece = units // shards
    got = [in_ref[s_ref[0] ^ k].astype(f32) for k in range(n)]
    for base, out_ref in ((0, gate_ref), (units, up_ref)):
        for i in range(shards):
            out_ref[:, i * n * piece : (i + 1) * n * piece] = jnp.concatenate(
                [got[k][:, base + i * piece : base + (i + 1) * piece] for k in range(n)], axis=1
            )


def unpick(s, pieces, shards, tile=64):
    n, rows, units = pieces.shape
    ffn = n * units // 2
    out = jax.ShapeDtypeStruct((rows, ffn), f32)
    return pl.pallas_call(
        functools.partial(unpick_kernel, shards=shards),
        grid_spec=pltpu.PrefetchScalarGridSpec(
            num_scalar_prefetch=1,
            grid=(rows // tile,),
            in_specs=[pl.BlockSpec((n, tile, units), lambda i, s: (0, i, 0))],
            out_specs=[pl.BlockSpec((tile, ffn), lambda i, s: (i, 0))] * 2,
        ),
        out_shape=[out, out],
        cost_estimate=pl.CostEstimate(
            flops=0, bytes_accessed=12 * rows * ffn, transcendentals=0),
        name="unpick",
    )(s.reshape(1), pieces)


def rope_tables(tokens):
    lane = jnp.arange(2 * HD, dtype=jnp.int32)[None, :] % HD
    turned = lane < ROT
    freq = ROPE_BASE ** (-((lane % HALF).astype(f32) * 2.0) / ROT)
    angle = jnp.arange(tokens, dtype=jnp.int32)[:, None].astype(f32) * freq
    sine = jnp.sin(angle)
    return (
        jnp.where(turned, jnp.cos(angle), 1.0),
        jnp.where(lane < HALF, -sine, 0.0),
        jnp.where(turned & (lane >= HALF), sine, 0.0),
    )


def body(
    hidden_in,
    cotangent,
    block_table,
    first_gain,
    first_bias,
    qkv_weight,
    qkv_bias,
    out_weight,
    second_gain,
    second_bias,
    gate_weight,
    up_weight,
    down_weight,
    *,
    n,
    fs,
):
    s = lax.axis_index("seq")
    f = lax.axis_index("fsdp")
    inputs = hidden_in[0].astype(f32)
    own, width = inputs.shape
    part = width // n
    rows = width // fs
    ffn = gate_weight.shape[1]
    units = ffn // n
    shard = ffn // fs
    piece = units // fs
    tokens = n * own
    order = [s ^ j for j in range(n)]

    blocks = jnp.concatenate(
        [lax.dynamic_slice_in_dim(block_table, order[j], 1, 0)[0] for j in range(n)]
    )
    ids = jnp.arange(2 * n, dtype=jnp.int32)
    slot = jnp.sum(jnp.where(blocks[None, :] == ids[:, None], ids[None, :], 0), axis=1)
    tables = rope_tables(tokens)

    def gather_fsdp(value):
        return lax.all_gather(value, "fsdp", axis=0, tiled=True)

    small = jnp.concatenate([first_gain, first_bias, second_gain, second_bias, qkv_bias])
    small = lax.all_gather(small, "fsdp", axis=0)
    vec = lambda i: small[:, i * rows : (i + 1) * rows].reshape(width).astype(f32)
    gain_one, bias_one, gain_two, bias_two = (vec(i) for i in range(4))
    bias_qkv = small[:, 4 * rows :].reshape(3, width).astype(f32)

    qkv_part = choose(
        s,
        [
            jnp.concatenate(
                [
                    qkv_weight[:, c * width + i * part : c * width + (i + 1) * part]
                    for c in range(3)
                ],
                axis=1,
            )
            for i in range(n)
        ],
    )
    w_qkv = gather_fsdp(qkv_part)

    normed_one, inverse_one = normalize(inputs)
    h1_own = (normed_one * gain_one + bias_one).astype(bf16)
    after = lambda value, first: lax.optimization_barrier((value, first))[0]
    slice_rows = rows // n
    w_out_part = gather_fsdp(
        after(lax.dynamic_slice_in_dim(out_weight, s * slice_rows, slice_rows, 0), h1_own)
    )
    picked = jnp.arange(units, dtype=jnp.int32)
    picked = (picked // piece) * shard + s * piece + picked % piece
    pick = (jnp.arange(ffn, dtype=jnp.int32)[:, None] == picked[None, :]).astype(bf16)
    pick = after(pick, h1_own)
    gate_up = jnp.concatenate(
        [
            jnp.dot(gate_weight, pick, preferred_element_type=f32).astype(bf16),
            jnp.dot(up_weight, pick, preferred_element_type=f32).astype(bf16),
        ],
        axis=1,
    )
    w_gate_up = gather_fsdp(gate_up)
    w_down = gather_fsdp(
        after(lax.dynamic_slice_in_dim(down_weight, s * piece, piece, 0), gate_up)
    )

    h1 = jnp.concatenate(gather_seq(h1_own, n), axis=0)
    bias_part = choose(s, [bias_qkv[:, i * part : (i + 1) * part] for i in range(n)])
    projected = jnp.dot(h1, w_qkv, preferred_element_type=f32) + bias_part.reshape(3 * part)
    head_out, lse, query, key, value = attend(slot, projected, tables)

    def natural(pieces):
        return [choose(s, [pieces[i ^ k] for i in range(n)]) for k in range(n)]

    def to_columns(pieces):
        return jnp.concatenate(natural(pieces), axis=1)

    def column_parts(value):
        return natural([value[:, k * part : (k + 1) * part] for k in range(n)])

    mixed = to_columns(
        exchange_seq([head_out[j * own : (j + 1) * own] for j in range(n)], n)
    )
    w_out = natural(
        [got.reshape(fs, 1, slice_rows, width) for got in gather_seq(w_out_part, n)]
    )
    w_out = jnp.concatenate(w_out, axis=1).reshape(width, width)
    residual = inputs + jnp.dot(mixed, w_out, preferred_element_type=f32)

    normed_two, inverse_two = normalize(residual)
    h2 = jnp.concatenate(
        gather_seq((normed_two * gain_two + bias_two).astype(bf16), n), axis=0
    )
    gate = jnp.dot(h2, w_gate_up, preferred_element_type=f32)
    gate, upward = gate[:, :units], gate[:, units:]
    sigmoid = jax.nn.sigmoid(gate)
    activated = (gate * sigmoid * upward).astype(bf16)
    branch = jnp.dot(activated, w_down, preferred_element_type=f32)
    branch = scatter_seq([branch[j * own : (j + 1) * own] for j in range(n)], n)
    block_out = (residual + branch).astype(bf16)

    d_own = cotangent[0]
    d_branch = jnp.concatenate(gather_seq(d_own, n), axis=0)
    across = (((1,), (1,)), ((), ()))
    down = (((0,), (0,)), ((), ()))
    dot = functools.partial(lax.dot_general, preferred_element_type=f32)

    def scatter_fsdp(value):
        return lax.psum_scatter(
            value.astype(bf16), "fsdp", scatter_dimension=0, tiled=True
        )

    down_term = dot(activated, d_branch, down).astype(bf16)
    down_grad = scatter_fsdp(down_term)
    d_activated = dot(after(d_branch, down_term), w_down, across)
    d_gate_up = jnp.concatenate(
        [
            (d_activated * upward * sigmoid * (1.0 + gate * (1.0 - sigmoid))).astype(bf16),
            (d_activated * gate * sigmoid).astype(bf16),
        ],
        axis=1,
    )
    gate_up_term = dot(h2, d_gate_up, down).astype(bf16)
    gate_up_grad = scatter_fsdp(gate_up_term)
    d_h2 = dot(after(d_gate_up, gate_up_term), w_gate_up, across)
    d_h2 = scatter_seq([d_h2[j * own : (j + 1) * own] for j in range(n)], n)
    gain_two_grad = jnp.sum(d_h2 * normed_two, axis=0)
    bias_two_grad = jnp.sum(d_h2, axis=0)
    d_residual = d_own.astype(f32) + norm_back(d_h2, normed_two, inverse_two, gain_two)

    d_attended = d_residual.astype(bf16)
    d_mixed = dot(d_attended, w_out, across).astype(bf16)
    d_mixed = jnp.concatenate(exchange_seq(column_parts(d_mixed), n), axis=0)
    d_projected = attend_back(
        slot, query, key, value, d_mixed, lse.transpose(0, 2, 1), tables
    )
    mixed_all = jnp.concatenate(gather_seq(mixed, n), axis=0)
    d_attended_part = jnp.concatenate(exchange_seq(column_parts(d_attended), n), axis=0)
    out_grad = scatter_fsdp(dot(mixed_all, d_attended_part, down))
    qkv_grad = scatter_fsdp(dot(h1, d_projected, down))
    qkv_bias_part = jnp.sum(d_projected.astype(f32), axis=0)
    d_h1 = dot(d_projected, w_qkv, across)
    d_h1 = scatter_seq([d_h1[j * own : (j + 1) * own] for j in range(n)], n)
    gain_one_grad = jnp.sum(d_h1 * normed_one, axis=0)
    bias_one_grad = jnp.sum(d_h1, axis=0)
    input_grad = (
        d_residual + norm_back(d_h1, normed_one, inverse_one, gain_one)
    ).astype(bf16)

    down_total = jnp.stack(natural(gather_seq(down_grad, n)))
    down_total = down_total.reshape(shard, width).astype(f32)
    out_total = to_columns(gather_seq(out_grad, n)).astype(f32)
    qkv_total = natural([got.reshape(rows, 3, part) for got in gather_seq(qkv_grad, n)])
    qkv_total = jnp.stack(qkv_total, axis=2).reshape(rows, 3 * width).astype(f32)
    gate_total, up_total = unpick(s, jnp.stack(gather_seq(gate_up_grad, n)), fs)

    bias_all = jnp.concatenate(
        [jnp.where(s == i, qkv_bias_part.reshape(3, part), 0.0) for i in range(n)], axis=1
    )
    sums = jnp.concatenate(
        [
            gain_one_grad.reshape(fs, rows),
            bias_one_grad.reshape(fs, rows),
            gain_two_grad.reshape(fs, rows),
            bias_two_grad.reshape(fs, rows),
            bias_all.reshape(fs, 3 * rows),
        ],
        axis=1,
    )
    sums = lax.psum(sums, ("fsdp", "seq"))
    sums = lax.dynamic_slice_in_dim(sums, f, 1, 0)[0]
    return (
        block_out[None],
        input_grad[None],
        sums[:rows],
        sums[rows : 2 * rows],
        qkv_total,
        sums[4 * rows :],
        out_total,
        sums[2 * rows : 3 * rows],
        sums[3 * rows : 4 * rows],
        gate_total,
        up_total,
        down_total,
    )


def solution(mesh):
    split = P("fsdp", None)
    act = P("fsdp", "seq", None)
    vec = P("fsdp")
    return jax.shard_map(
        functools.partial(body, n=mesh.shape["seq"], fs=mesh.shape["fsdp"]),
        mesh=mesh,
        in_specs=(act, act, P(), vec, vec, split, vec, split, vec, vec, split, split, split),
        out_specs=(act, act, vec, vec, split, vec, split, vec, vec, split, split, split),
        check_vma=False,
    )
```

```python
import functools

import jax
import jax.numpy as jnp
from jax import lax
from jax.experimental import pallas as pl
from jax.experimental.pallas import tpu as pltpu
from jax.sharding import PartitionSpec as P


HD = 64
ROT = HD // 4
HALF = ROT // 2
EPS = 1e-05
ROPE_BASE = 10000.0
NEG = -1e30
SCALE = float(HD) ** -0.5
f32 = jnp.float32
bf16 = jnp.bfloat16


def normalize(values):
    centred = values - jnp.mean(values, axis=-1, keepdims=True)
    inverse = lax.rsqrt(jnp.mean(centred * centred, axis=-1, keepdims=True) + EPS)
    return (centred * inverse, inverse)


def norm_back(d_normed, normed, inverse, gain):
    scaled = d_normed * gain
    return inverse * (
        scaled
        - jnp.mean(scaled, axis=-1, keepdims=True)
        - normed * jnp.mean(scaled * normed, axis=-1, keepdims=True)
    )


def swap(value, mask, n):
    return lax.ppermute(value, "seq", [(i, i ^ mask) for i in range(n)])


def halves(count):
    middle = (count // 2 + 8) // 16 * 16
    return ((0, middle), (middle, count))


def gather_streams(value, n):
    bits = n.bit_length() - 1
    streams = [{0: value[first:last]} for first, last in halves(value.shape[0])]
    for step in range(bits):
        for index, have in enumerate(streams):
            mask = 1 << ((index + step) % bits)
            have.update({key ^ mask: swap(item, mask, n) for key, item in have.items()})
    return [[have[j] for j in range(n)] for have in streams]


def gather_seq(value, n):
    return [jnp.concatenate(pair, axis=0) for pair in zip(*gather_streams(value, n))]


def scatter_seq(pieces, n):
    bits = n.bit_length() - 1
    streams = [
        {j: pieces[j][first:last] for j in range(n)}
        for first, last in halves(pieces[0].shape[0])
    ]
    for step in range(bits):
        for index, have in enumerate(streams):
            mask = 1 << ((index + bits - 1 - step) % bits)
            got = {
                key ^ mask: swap(item.astype(bf16), mask, n)
                for key, item in have.items()
                if key & mask
            }
            streams[index] = {
                key: item + got[key].astype(f32)
                for key, item in have.items()
                if not key & mask
            }
    return jnp.concatenate([have[0] for have in streams], axis=0)


def exchange_seq(pieces, n):
    return [pieces[0]] + [swap(pieces[j], j, n) for j in range(1, n)]


def spread_seq(value, n):
    return exchange_seq([value] * n, n)


def collect_seq(pieces, n):
    got = exchange_seq([pieces[0]] + [piece.astype(bf16) for piece in pieces[1:]], n)
    return sum(item.astype(f32) for item in got)


def choose(index, options):
    out = options[0]
    for i, option in enumerate(options[1:], 1):
        out = jnp.where(index == i, option, out)
    return out


def turn(tensor, cosine, left, right, sign):
    back = pltpu.roll(tensor, 2 * HD - HALF, 1)
    ahead = pltpu.roll(tensor, HALF, 1)
    return tensor * cosine + sign * (back * left + ahead * right)


def attend_kernel(slot_ref, q_ref, k_ref, v_ref, cos_ref, left_ref, right_ref,
                  o_ref, lse_ref, qo_ref, ko_ref, vo_ref, tile):
    tokens = q_ref.shape[0]
    slots = slot_ref.shape[0]
    blk = tokens // slots
    for p in range(slots):
        rows = pl.ds(pl.multiple_of(slot_ref[p] * blk, blk), blk)
        own = pl.ds(p * blk, blk)
        cosine, left, right = cos_ref[own, :], left_ref[own, :], right_ref[own, :]
        qo_ref[own, :] = turn(q_ref[rows, :], cosine, left, right, 1.0).astype(bf16)
        ko_ref[own, :] = turn(k_ref[rows, :], cosine, left, right, 1.0).astype(bf16)
        vo_ref[own, :] = v_ref[rows, :].astype(bf16)
    mask = lax.broadcasted_iota(jnp.int32, (tile, tile), 1) <= lax.broadcasted_iota(
        jnp.int32, (tile, tile), 0
    )
    for t in range(tokens // tile):
        own = pl.ds(t * tile, tile)
        outs, stats = [], []
        for h in range(2):
            lanes = pl.ds(h * HD, HD)
            query = qo_ref[own, lanes]
            end = (t + 1) * tile
            scores = lax.dot_general(
                query, ko_ref[pl.ds(0, end), lanes], (((1,), (1,)), ((), ())),
                preferred_element_type=f32) * SCALE
            diag = jnp.where(mask, scores[:, t * tile :], NEG)
            scores = jnp.concatenate([scores[:, : t * tile], diag], axis=1) if t else diag
            peak = jnp.max(scores, axis=1, keepdims=True)
            weights = jnp.exp(scores - peak)
            total = jnp.sum(weights, axis=1, keepdims=True)
            weights = (weights * (1.0 / total)).astype(bf16)
            outs.append(jnp.dot(weights, vo_ref[pl.ds(0, end), lanes],
                                preferred_element_type=f32))
            stats.append(peak + jnp.log(total))
        out = jnp.concatenate(outs, axis=1).astype(bf16)
        lse_ref[0, own, :] = jnp.concatenate(stats, axis=1)
        for part in range(tile // blk):
            rows = pl.ds(pl.multiple_of(slot_ref[t * (tile // blk) + part] * blk, blk), blk)
            o_ref[rows, :] = out[part * blk : (part + 1) * blk]


def attend(slot, projected, tables, tile=256):
    tokens, width = projected.shape
    width //= 3
    groups = width // (2 * HD)
    lanes = 2 * HD
    col = lambda base: pl.BlockSpec((tokens, lanes), lambda i, s: (0, base + i))
    table = pl.BlockSpec((tokens, lanes), lambda i, s: (0, 0))
    return pl.pallas_call(
        functools.partial(attend_kernel, tile=tile),
        grid_spec=pltpu.PrefetchScalarGridSpec(
            num_scalar_prefetch=1,
            grid=(groups,),
            in_specs=[col(0), col(groups), col(2 * groups), table, table, table],
            out_specs=[col(0), pl.BlockSpec((1, tokens, 2), lambda i, s: (i, 0, 0)),
                       col(0), col(0), col(0)],
        ),
        out_shape=[
            jax.ShapeDtypeStruct((tokens, width), bf16),
            jax.ShapeDtypeStruct((groups, tokens, 2), f32),
            jax.ShapeDtypeStruct((tokens, width), bf16),
            jax.ShapeDtypeStruct((tokens, width), bf16),
            jax.ShapeDtypeStruct((tokens, width), bf16),
        ],
        cost_estimate=pl.CostEstimate(
            flops=4 * tokens * tokens * width, bytes_accessed=24 * tokens * width,
            transcendentals=tokens * tokens * 2 * groups),
        name="attend",
    )(slot, projected, projected, projected, *tables)


def attend_back_kernel(slot_ref, q_ref, k_ref, v_ref, d_ref, lse_ref,
                       cos_ref, left_ref, right_ref, g_ref,
                       d_pos, dq_acc, dk_acc, dv_acc, tile):
    tokens = q_ref.shape[0]
    slots = slot_ref.shape[0]
    blk = tokens // slots
    width = g_ref.shape[1] // 3
    group = pl.program_id(0)
    for p in range(slots):
        rows = pl.ds(pl.multiple_of(slot_ref[p] * blk, blk), blk)
        d_pos[pl.ds(p * blk, blk), :] = d_ref[rows, :]
    dk_acc[...] = jnp.zeros_like(dk_acc)
    dv_acc[...] = jnp.zeros_like(dv_acc)
    mask = lax.broadcasted_iota(jnp.int32, (tile, tile), 0) <= lax.broadcasted_iota(
        jnp.int32, (tile, tile), 1
    )
    for t in range(tokens // tile):
        own = pl.ds(t * tile, tile)
        past = pl.ds(0, (t + 1) * tile)
        grads = []
        keys_grad, values_grad = [], []
        for h in range(2):
            lanes = pl.ds(h * HD, HD)
            query, keys = q_ref[own, lanes], k_ref[past, lanes]
            d_out = d_pos[own, lanes]
            scores = lax.dot_general(keys, query, (((1,), (1,)), ((), ())),
                                     preferred_element_type=f32) * SCALE
            diag = jnp.where(mask, scores[t * tile :], NEG)
            scores = jnp.concatenate([scores[: t * tile], diag], axis=0) if t else diag
            probs = jnp.exp(scores - lse_ref[0, pl.ds(h, 1), own])
            d_probs = lax.dot_general(v_ref[past, lanes], d_out, (((1,), (1,)), ((), ())),
                                      preferred_element_type=f32)
            delta = jnp.sum(d_probs * probs, axis=0, keepdims=True)
            d_scores = (probs * (d_probs - delta)).astype(bf16)
            values_grad.append(jnp.dot(probs.astype(bf16), d_out, preferred_element_type=f32))
            keys_grad.append(jnp.dot(d_scores, query, preferred_element_type=f32))
            grads.append(lax.dot_general(d_scores, keys, (((0,), (0,)), ((), ())),
                                         preferred_element_type=f32))
        dk_acc[past, :] += jnp.concatenate(keys_grad, axis=1)
        dv_acc[past, :] += jnp.concatenate(values_grad, axis=1)
        dq_acc[own, :] = jnp.concatenate(grads, axis=1)
    lanes = 2 * HD
    for p in range(slots):
        rows = pl.ds(pl.multiple_of(slot_ref[p] * blk, blk), blk)
        own = pl.ds(p * blk, blk)
        cosine, left, right = cos_ref[own, :], left_ref[own, :], right_ref[own, :]
        first = pl.multiple_of(group * lanes, lanes)
        g_ref[rows, pl.ds(first, lanes)] = turn(
            dq_acc[own, :] * SCALE, cosine, left, right, -1.0).astype(bf16)
        g_ref[rows, pl.ds(width + first, lanes)] = turn(
            dk_acc[own, :] * SCALE, cosine, left, right, -1.0).astype(bf16)
        g_ref[rows, pl.ds(2 * width + first, lanes)] = dv_acc[own, :].astype(bf16)


def attend_back(slot, query, key, value, d_mixed, lse, tables, tile=256):
    tokens, width = query.shape
    groups = width // (2 * HD)
    lanes = 2 * HD
    col = pl.BlockSpec((tokens, lanes), lambda i, s: (0, i))
    table = pl.BlockSpec((tokens, lanes), lambda i, s: (0, 0))
    return pl.pallas_call(
        functools.partial(attend_back_kernel, tile=tile),
        grid_spec=pltpu.PrefetchScalarGridSpec(
            num_scalar_prefetch=1,
            grid=(groups,),
            in_specs=[col, col, col, col,
                      pl.BlockSpec((1, 2, tokens), lambda i, s: (i, 0, 0)),
                      table, table, table],
            out_specs=pl.BlockSpec((tokens, 3 * width), lambda i, s: (0, 0)),
            scratch_shapes=[pltpu.VMEM((tokens, lanes), bf16)]
            + [pltpu.VMEM((tokens, lanes), f32)] * 3,
        ),
        out_shape=jax.ShapeDtypeStruct((tokens, 3 * width), bf16),
        cost_estimate=pl.CostEstimate(
            flops=10 * tokens * tokens * width, bytes_accessed=16 * tokens * width,
            transcendentals=tokens * tokens * 2 * groups),
        name="attend_back",
    )(slot, query, key, value, d_mixed, lse, *tables)


def finish_kernel(s_ref, *refs, n, steps, outs, place):
    ins, out_refs = refs[:-outs], refs[-outs:]
    for stream in range(len(ins) // n):
        group = ins[stream * n : (stream + 1) * n]

        @pl.when(pl.program_id(0) // steps == stream)
        def _():
            got = [item[...] for item in group]
            place([choose(s_ref[0], [got[i ^ k] for i in range(n)]) for k in range(n)], out_refs)


def finish(s, streams, widths, place, tile):
    n = len(streams[0])
    count, columns = streams[0][0].shape
    steps = count // tile
    rows = count * len(streams)
    specs = []
    for index in range(len(streams)):
        spec = pl.BlockSpec(
            (tile, columns),
            lambda i, s, index=index: (jnp.clip(i - index * steps, 0, steps - 1), 0),
        )
        specs += [spec] * n
    return pl.pallas_call(
        functools.partial(
            finish_kernel, n=n, steps=steps, outs=len(widths), place=place
        ),
        grid_spec=pltpu.PrefetchScalarGridSpec(
            num_scalar_prefetch=1,
            grid=(steps * len(streams),),
            in_specs=specs,
            out_specs=[pl.BlockSpec((tile, width), lambda i, s: (i, 0)) for width in widths],
        ),
        out_shape=[jax.ShapeDtypeStruct((rows, width), f32) for width in widths],
        cost_estimate=pl.CostEstimate(
            flops=0, bytes_accessed=6 * rows * sum(widths), transcendentals=0),
    )(s.reshape(1), *[item for group in streams for item in group])


def place_columns(parts, pieces, outs):
    width = pieces[0].shape[1] // parts
    for c in range(parts):
        for k, item in enumerate(pieces):
            first = (c * len(pieces) + k) * width
            outs[0][:, first : first + width] = item[:, c * width : (c + 1) * width].astype(f32)


def place_units(shards, pieces, outs):
    units = pieces[0].shape[1] // 2
    piece = units // shards
    wide = piece * len(pieces)
    pieces = [item.astype(f32) for item in pieces]
    for base, out in zip((0, units), outs):
        for i in range(shards):
            first = base + i * piece
            out[:, i * wide : (i + 1) * wide] = jnp.concatenate(
                [item[:, first : first + piece] for item in pieces], axis=1
            )


def rope_tables(tokens):
    lane = jnp.arange(2 * HD, dtype=jnp.int32)[None, :] % HD
    turned = lane < ROT
    freq = ROPE_BASE ** (-((lane % HALF).astype(f32) * 2.0) / ROT)
    angle = jnp.arange(tokens, dtype=jnp.int32)[:, None].astype(f32) * freq
    sine = jnp.sin(angle)
    return (
        jnp.where(turned, jnp.cos(angle), 1.0),
        jnp.where(lane < HALF, -sine, 0.0),
        jnp.where(turned & (lane >= HALF), sine, 0.0),
    )


def body(
    hidden_in,
    cotangent,
    block_table,
    first_gain,
    first_bias,
    qkv_weight,
    qkv_bias,
    out_weight,
    second_gain,
    second_bias,
    gate_weight,
    up_weight,
    down_weight,
    *,
    n,
    fs,
):
    s = lax.axis_index("seq")
    inputs = hidden_in[0].astype(f32)
    own, width = inputs.shape
    part = width // n
    rows = width // fs
    ffn = gate_weight.shape[1]
    units = ffn // n
    shard = ffn // fs
    piece = units // fs
    tokens = n * own
    order = [s ^ j for j in range(n)]

    blocks = jnp.concatenate(
        [lax.dynamic_slice_in_dim(block_table, order[j], 1, 0)[0] for j in range(n)]
    )
    ids = jnp.arange(2 * n, dtype=jnp.int32)
    slot = jnp.sum(jnp.where(blocks[None, :] == ids[:, None], ids[None, :], 0), axis=1)
    tables = rope_tables(tokens)

    def gather_fsdp(value):
        return lax.all_gather(value, "fsdp", axis=0, tiled=True)

    after = lambda value, first: lax.optimization_barrier((value, first))[0]

    small = jnp.concatenate([first_gain, first_bias, second_gain, second_bias, qkv_bias])
    small = lax.all_gather(small, "fsdp", axis=0)
    vec = lambda i: small[:, i * rows : (i + 1) * rows].reshape(width).astype(f32)
    gain_one, bias_one, gain_two, bias_two = (vec(i) for i in range(4))
    bias_qkv = small[:, 4 * rows :].reshape(3, width).astype(f32)

    qkv_part = choose(
        s,
        [
            jnp.concatenate(
                [
                    qkv_weight[:, c * width + i * part : c * width + (i + 1) * part]
                    for c in range(3)
                ],
                axis=1,
            )
            for i in range(n)
        ],
    )
    out_part = choose(s, [out_weight[:, i * part : (i + 1) * part] for i in range(n)])
    w_first = gather_fsdp(jnp.concatenate([qkv_part, out_part], axis=1))
    w_qkv = w_first[:, : 3 * part]

    normed_one, inverse_one = normalize(inputs)
    h1_own = (normed_one * gain_one + bias_one).astype(bf16)
    picked = jnp.arange(units, dtype=jnp.int32)
    picked = (picked // piece) * shard + s * piece + picked % piece
    picked = after(picked, h1_own)
    pick = (jnp.arange(ffn, dtype=jnp.int32)[:, None] == picked[None, :]).astype(bf16)
    gate_up = jnp.concatenate(
        [
            jnp.dot(gate_weight, pick, preferred_element_type=f32).astype(bf16),
            jnp.dot(up_weight, pick, preferred_element_type=f32).astype(bf16),
        ],
        axis=1,
    )
    w_gate_up = gather_fsdp(gate_up)
    w_down = gather_fsdp(choose(s, [down_weight[i * piece : (i + 1) * piece] for i in range(n)]))

    h1 = jnp.concatenate(gather_seq(h1_own, n), axis=0)
    core = lax.axis_index("fsdp") % 2
    half = width // 2
    w_out_half = choose(core, [w_first[:half, 3 * part :], w_first[half:, 3 * part :]])
    w_out_pieces = gather_seq(after(w_out_half, h1), n)
    bias_part = choose(s, [bias_qkv[:, i * part : (i + 1) * part] for i in range(n)])
    projected = jnp.dot(h1, w_qkv, preferred_element_type=f32)
    projected = projected + bias_part.reshape(3 * part)
    head_out, lse, query, key, value = attend(slot, projected, tables)

    def natural(pieces):
        return [choose(s, [pieces[i ^ k] for i in range(n)]) for k in range(n)]

    def to_columns(pieces):
        return jnp.concatenate(natural(pieces), axis=1)

    def column_parts(value):
        return natural([value[:, k * part : (k + 1) * part] for k in range(n)])

    mixed = to_columns(
        exchange_seq([head_out[j * own : (j + 1) * own] for j in range(n)], n)
    )
    w_out = to_columns(w_out_pieces)
    w_out = [w_out, lax.ppermute(w_out, "fsdp", [(i, i ^ 1) for i in range(fs)])]
    by_core = lambda a, b: [jnp.where(core == 0, a, b), jnp.where(core == 0, b, a)]
    mixed_first, mixed_second = by_core(mixed[:, :half], mixed[:, half:])
    residual = (
        inputs
        + jnp.dot(mixed_first, w_out[0], preferred_element_type=f32)
        + jnp.dot(mixed_second, w_out[1], preferred_element_type=f32)
    )

    normed_two, inverse_two = normalize(residual)
    h2 = jnp.concatenate(gather_seq((normed_two * gain_two + bias_two).astype(bf16), n), axis=0)
    d_own = cotangent[0]
    d_branch = jnp.concatenate(gather_seq(after(d_own, h2), n), axis=0)
    gate = jnp.dot(h2, w_gate_up, preferred_element_type=f32)
    gate, upward = gate[:, :units], gate[:, units:]
    sigmoid = jax.nn.sigmoid(gate)
    activated = (gate * sigmoid * upward).astype(bf16)
    across = (((1,), (1,)), ((), ()))
    down = (((0,), (0,)), ((), ()))
    dot = functools.partial(lax.dot_general, preferred_element_type=f32)

    def scatter_fsdp(value):
        return lax.psum_scatter(value, "fsdp", scatter_dimension=0, tiled=True)

    down_term = dot(activated, d_branch, down).astype(bf16)
    down_grad = scatter_fsdp(down_term)
    mixed_all = jnp.concatenate(gather_seq(after(mixed, d_branch), n), axis=0)
    branch = dot(after(activated, down_term), w_down, (((1,), (0,)), ((), ())))
    d_activated = dot(after(d_branch, branch), w_down, across)
    branch = collect_seq([branch[j * own : (j + 1) * own] for j in range(n)], n)
    block_out = (residual + branch).astype(bf16)
    d_gate_up = jnp.concatenate(
        [
            (d_activated * upward * sigmoid * (1.0 + gate * (1.0 - sigmoid))).astype(bf16),
            (d_activated * gate * sigmoid).astype(bf16),
        ],
        axis=1,
    )
    gate_up_term = dot(h2, d_gate_up, down).astype(bf16)
    gate_up_grad = scatter_fsdp(gate_up_term)
    d_h2 = dot(after(d_gate_up, gate_up_term), w_gate_up, across)
    d_h2 = scatter_seq([d_h2[j * own : (j + 1) * own] for j in range(n)], n)
    gain_two_grad = jnp.sum(d_h2 * normed_two, axis=0)
    bias_two_grad = jnp.sum(d_h2, axis=0)
    d_residual = d_own.astype(f32) + norm_back(d_h2, normed_two, inverse_two, gain_two)

    d_attended = d_residual.astype(bf16)
    d_mixed = by_core(*[dot(d_attended, item, across).astype(bf16) for item in w_out])
    d_mixed = jnp.concatenate(d_mixed, axis=1)
    d_mixed = jnp.concatenate(exchange_seq(column_parts(d_mixed), n), axis=0)
    d_projected = attend_back(
        slot, query, key, value, d_mixed, lse.transpose(0, 2, 1), tables
    )
    d_attended_part = exchange_seq(column_parts(after(d_attended, d_mixed)), n)
    d_attended_part = jnp.concatenate(d_attended_part, axis=0)
    down_pieces = spread_seq(after(down_grad, d_mixed), n)
    out_term = dot(mixed_all, d_attended_part, down).astype(bf16)
    qkv_term = dot(h1, d_projected, down).astype(bf16)
    qkv_grad = scatter_fsdp(qkv_term)
    qkv_bias_part = jnp.sum(d_projected.astype(f32), axis=0)
    d_h1 = dot(after(d_projected, qkv_term), w_qkv, across)
    d_h1 = scatter_seq([d_h1[j * own : (j + 1) * own] for j in range(n)], n)
    gain_one_grad = jnp.sum(d_h1 * normed_one, axis=0)
    bias_one_grad = jnp.sum(d_h1, axis=0)
    input_grad = (
        d_residual + norm_back(d_h1, normed_one, inverse_one, gain_one)
    ).astype(bf16)

    bias_all = jnp.concatenate(
        [jnp.where(s == i, qkv_bias_part.reshape(3, part), 0.0) for i in range(n)], axis=1
    )
    small = [
        gain_one_grad.reshape(fs, rows),
        bias_one_grad.reshape(fs, rows),
        gain_two_grad.reshape(fs, rows),
        bias_two_grad.reshape(fs, rows),
        bias_all.reshape(fs, 3 * rows),
    ]
    extra = -(-7 * rows // part)
    extra += -extra % 16
    small.append(jnp.zeros((fs, extra * part - 7 * rows), f32))
    small = jnp.concatenate(small, axis=1).astype(bf16).reshape(fs, extra, part)
    out_term = jnp.concatenate([out_term.reshape(fs, rows, part), small], axis=1)
    out_grad = scatter_fsdp(out_term.reshape(fs * (rows + extra), part))

    down_total = jnp.stack(natural(down_pieces)).reshape(shard, width).astype(f32)
    gate_up_pieces = gather_streams(after(gate_up_grad, d_h1), n)
    gate_total, up_total = finish(
        s, gate_up_pieces, (ffn, ffn),
        functools.partial(place_units, fs), min(64, rows // 2))
    qkv_pieces = gather_streams(after(qkv_grad, gate_up_pieces[0][n - 1]), n)
    (qkv_total,) = finish(
        s, qkv_pieces, (3 * width,),
        functools.partial(place_columns, 3), min(64, rows // 2))
    out_pieces = spread_seq(out_grad, n)
    (out_total,) = finish(
        s, [[got[:rows] for got in out_pieces]], (width,),
        functools.partial(place_columns, 1), rows)
    sums = sum(got[rows:].astype(f32) for got in out_pieces).reshape(extra * part)
    return (
        block_out[None],
        input_grad[None],
        sums[:rows],
        sums[rows : 2 * rows],
        qkv_total,
        sums[4 * rows : 7 * rows],
        out_total,
        sums[2 * rows : 3 * rows],
        sums[3 * rows : 4 * rows],
        gate_total,
        up_total,
        down_total,
    )


def solution(mesh):
    split = P("fsdp", None)
    act = P("fsdp", "seq", None)
    vec = P("fsdp")
    return jax.shard_map(
        functools.partial(body, n=mesh.shape["seq"], fs=mesh.shape["fsdp"]),
        mesh=mesh,
        in_specs=(act, act, P(), vec, vec, split, vec, split, vec, vec, split, split, split),
        out_specs=(act, act, vec, vec, split, vec, split, vec, vec, split, split, split),
        check_vma=False,
    )
```

```python
import functools

import jax
import jax.numpy as jnp
from jax import lax
from jax.experimental import pallas as pl
from jax.experimental.pallas import tpu as pltpu
from jax.sharding import PartitionSpec as P


HD = 64
ROT = HD // 4
HALF = ROT // 2
EPS = 1e-05
ROPE_BASE = 10000.0
NEG = -1e30
SCALE = float(HD) ** -0.5
f32 = jnp.float32
bf16 = jnp.bfloat16


def normalize(values):
    centred = values - jnp.mean(values, axis=-1, keepdims=True)
    inverse = lax.rsqrt(jnp.mean(centred * centred, axis=-1, keepdims=True) + EPS)
    return (centred * inverse, inverse)


def norm_back(d_normed, normed, inverse, gain):
    scaled = d_normed * gain
    return inverse * (
        scaled
        - jnp.mean(scaled, axis=-1, keepdims=True)
        - normed * jnp.mean(scaled * normed, axis=-1, keepdims=True)
    )


def swap(value, mask, n):
    return lax.ppermute(value, "seq", [(i, i ^ mask) for i in range(n)])


def after(value, first):
    return lax.optimization_barrier((value, first))[0]


def halves(count):
    middle = (count // 2 + 8) // 16 * 16
    return ((0, middle), (middle, count))


def gather_streams(value, n, second=None):
    bits = n.bit_length() - 1
    streams = [{0: value[first:last]} for first, last in halves(value.shape[0])]
    for step in range(bits):
        for index, have in enumerate(streams):
            mask = 1 << ((index + step) % bits)
            items = have
            if step:
                last = list(have)[-1]
                items = {k: after(v, have[last]) for k, v in have.items() if k != last}
                items[last] = have[last]
                if second is not None:
                    items = {k: after(v, second) for k, v in items.items()}
            have.update({key ^ mask: swap(item, mask, n) for key, item in items.items()})
    return [[have[j] for j in range(n)] for have in streams]


def gather_seq(value, n):
    return [jnp.concatenate(pair, axis=0) for pair in zip(*gather_streams(value, n))]


def scatter_seq(pieces, n):
    bits = n.bit_length() - 1
    streams = [
        {j: pieces[j][first:last] for j in range(n)}
        for first, last in halves(pieces[0].shape[0])
    ]
    for step in range(bits):
        for index, have in enumerate(streams):
            mask = 1 << ((index + bits - 1 - step) % bits)
            got = {
                key ^ mask: swap(item.astype(bf16), mask, n)
                for key, item in have.items()
                if key & mask
            }
            streams[index] = {
                key: item + got[key].astype(f32)
                for key, item in have.items()
                if not key & mask
            }
    return jnp.concatenate([have[0] for have in streams], axis=0)


def exchange_seq(pieces, n):
    return [pieces[0]] + [swap(pieces[j], j, n) for j in range(1, n)]


def spread_seq(value, n):
    return exchange_seq([value] * n, n)


def collect_seq(pieces, n):
    got = exchange_seq([pieces[0]] + [piece.astype(bf16) for piece in pieces[1:]], n)
    return sum(item.astype(f32) for item in got)


def choose(index, options):
    out = options[0]
    for i, option in enumerate(options[1:], 1):
        out = jnp.where(index == i, option, out)
    return out


def turn(tensor, cosine, left, right, sign):
    back = pltpu.roll(tensor, 2 * HD - HALF, 1)
    ahead = pltpu.roll(tensor, HALF, 1)
    return tensor * cosine + sign * (back * left + ahead * right)


def attend_kernel(slot_ref, q_ref, k_ref, v_ref, cos_ref, left_ref, right_ref,
                  o_ref, lse_ref, qo_ref, ko_ref, vo_ref, tile):
    tokens = q_ref.shape[0]
    slots = slot_ref.shape[0]
    blk = tokens // slots
    for p in range(slots):
        rows = pl.ds(pl.multiple_of(slot_ref[p] * blk, blk), blk)
        own = pl.ds(p * blk, blk)
        cosine, left, right = cos_ref[own, :], left_ref[own, :], right_ref[own, :]
        qo_ref[own, :] = turn(q_ref[rows, :], cosine, left, right, 1.0).astype(bf16)
        ko_ref[own, :] = turn(k_ref[rows, :], cosine, left, right, 1.0).astype(bf16)
        vo_ref[own, :] = v_ref[rows, :].astype(bf16)
    mask = lax.broadcasted_iota(jnp.int32, (tile, tile), 1) <= lax.broadcasted_iota(
        jnp.int32, (tile, tile), 0
    )
    for t in range(tokens // tile):
        own = pl.ds(t * tile, tile)
        outs, stats = [], []
        for h in range(2):
            lanes = pl.ds(h * HD, HD)
            query = qo_ref[own, lanes]
            end = (t + 1) * tile
            scores = lax.dot_general(
                query, ko_ref[pl.ds(0, end), lanes], (((1,), (1,)), ((), ())),
                preferred_element_type=f32) * SCALE
            diag = jnp.where(mask, scores[:, t * tile :], NEG)
            scores = jnp.concatenate([scores[:, : t * tile], diag], axis=1) if t else diag
            peak = jnp.max(scores, axis=1, keepdims=True)
            weights = jnp.exp(scores - peak)
            total = jnp.sum(weights, axis=1, keepdims=True)
            weights = (weights * (1.0 / total)).astype(bf16)
            outs.append(jnp.dot(weights, vo_ref[pl.ds(0, end), lanes],
                                preferred_element_type=f32))
            stats.append(peak + jnp.log(total))
        out = jnp.concatenate(outs, axis=1).astype(bf16)
        lse_ref[0, own, :] = jnp.concatenate(stats, axis=1)
        for part in range(tile // blk):
            rows = pl.ds(pl.multiple_of(slot_ref[t * (tile // blk) + part] * blk, blk), blk)
            o_ref[rows, :] = out[part * blk : (part + 1) * blk]


def attend(slot, projected, tables, tile=256):
    tokens, width = projected.shape
    width //= 3
    groups = width // (2 * HD)
    lanes = 2 * HD
    col = lambda base: pl.BlockSpec((tokens, lanes), lambda i, s: (0, base + i))
    table = pl.BlockSpec((tokens, lanes), lambda i, s: (0, 0))
    return pl.pallas_call(
        functools.partial(attend_kernel, tile=tile),
        grid_spec=pltpu.PrefetchScalarGridSpec(
            num_scalar_prefetch=1,
            grid=(groups,),
            in_specs=[col(0), col(groups), col(2 * groups), table, table, table],
            out_specs=[col(0), pl.BlockSpec((1, tokens, 2), lambda i, s: (i, 0, 0)),
                       col(0), col(0), col(0)],
        ),
        out_shape=[
            jax.ShapeDtypeStruct((tokens, width), bf16),
            jax.ShapeDtypeStruct((groups, tokens, 2), f32),
            jax.ShapeDtypeStruct((tokens, width), bf16),
            jax.ShapeDtypeStruct((tokens, width), bf16),
            jax.ShapeDtypeStruct((tokens, width), bf16),
        ],
        cost_estimate=pl.CostEstimate(
            flops=4 * tokens * tokens * width, bytes_accessed=24 * tokens * width,
            transcendentals=tokens * tokens * 2 * groups),
        name="attend",
    )(slot, projected, projected, projected, *tables)


def attend_back_kernel(slot_ref, q_ref, k_ref, v_ref, d_ref, lse_ref,
                       cos_ref, left_ref, right_ref, g_ref,
                       d_pos, dq_acc, dk_acc, dv_acc, tile):
    tokens = q_ref.shape[0]
    slots = slot_ref.shape[0]
    blk = tokens // slots
    width = g_ref.shape[1] // 3
    group = pl.program_id(0)
    for p in range(slots):
        rows = pl.ds(pl.multiple_of(slot_ref[p] * blk, blk), blk)
        d_pos[pl.ds(p * blk, blk), :] = d_ref[rows, :]
    dk_acc[...] = jnp.zeros_like(dk_acc)
    dv_acc[...] = jnp.zeros_like(dv_acc)
    mask = lax.broadcasted_iota(jnp.int32, (tile, tile), 0) <= lax.broadcasted_iota(
        jnp.int32, (tile, tile), 1
    )
    for t in range(tokens // tile):
        own = pl.ds(t * tile, tile)
        past = pl.ds(0, (t + 1) * tile)
        grads = []
        keys_grad, values_grad = [], []
        for h in range(2):
            lanes = pl.ds(h * HD, HD)
            query, keys = q_ref[own, lanes], k_ref[past, lanes]
            d_out = d_pos[own, lanes]
            scores = lax.dot_general(keys, query, (((1,), (1,)), ((), ())),
                                     preferred_element_type=f32) * SCALE
            diag = jnp.where(mask, scores[t * tile :], NEG)
            scores = jnp.concatenate([scores[: t * tile], diag], axis=0) if t else diag
            probs = jnp.exp(scores - lse_ref[0, pl.ds(h, 1), own])
            d_probs = lax.dot_general(v_ref[past, lanes], d_out, (((1,), (1,)), ((), ())),
                                      preferred_element_type=f32)
            delta = jnp.sum(d_probs * probs, axis=0, keepdims=True)
            d_scores = (probs * (d_probs - delta)).astype(bf16)
            values_grad.append(jnp.dot(probs.astype(bf16), d_out, preferred_element_type=f32))
            keys_grad.append(jnp.dot(d_scores, query, preferred_element_type=f32))
            grads.append(lax.dot_general(d_scores, keys, (((0,), (0,)), ((), ())),
                                         preferred_element_type=f32))
        dk_acc[past, :] += jnp.concatenate(keys_grad, axis=1)
        dv_acc[past, :] += jnp.concatenate(values_grad, axis=1)
        dq_acc[own, :] = jnp.concatenate(grads, axis=1)
    lanes = 2 * HD
    for p in range(slots):
        rows = pl.ds(pl.multiple_of(slot_ref[p] * blk, blk), blk)
        own = pl.ds(p * blk, blk)
        cosine, left, right = cos_ref[own, :], left_ref[own, :], right_ref[own, :]
        first = pl.multiple_of(group * lanes, lanes)
        g_ref[rows, pl.ds(first, lanes)] = turn(
            dq_acc[own, :] * SCALE, cosine, left, right, -1.0).astype(bf16)
        g_ref[rows, pl.ds(width + first, lanes)] = turn(
            dk_acc[own, :] * SCALE, cosine, left, right, -1.0).astype(bf16)
        g_ref[rows, pl.ds(2 * width + first, lanes)] = dv_acc[own, :].astype(bf16)


def attend_back(slot, query, key, value, d_mixed, lse, tables, tile=256):
    tokens, width = query.shape
    groups = width // (2 * HD)
    lanes = 2 * HD
    col = pl.BlockSpec((tokens, lanes), lambda i, s: (0, i))
    table = pl.BlockSpec((tokens, lanes), lambda i, s: (0, 0))
    return pl.pallas_call(
        functools.partial(attend_back_kernel, tile=tile),
        grid_spec=pltpu.PrefetchScalarGridSpec(
            num_scalar_prefetch=1,
            grid=(groups,),
            in_specs=[col, col, col, col,
                      pl.BlockSpec((1, 2, tokens), lambda i, s: (i, 0, 0)),
                      table, table, table],
            out_specs=pl.BlockSpec((tokens, 3 * width), lambda i, s: (0, 0)),
            scratch_shapes=[pltpu.VMEM((tokens, lanes), bf16)]
            + [pltpu.VMEM((tokens, lanes), f32)] * 3,
        ),
        out_shape=jax.ShapeDtypeStruct((tokens, 3 * width), bf16),
        cost_estimate=pl.CostEstimate(
            flops=10 * tokens * tokens * width, bytes_accessed=16 * tokens * width,
            transcendentals=tokens * tokens * 2 * groups),
        name="attend_back",
    )(slot, query, key, value, d_mixed, lse, *tables)


def feed_kernel(h_ref, w_ref, both_ref, act_ref):
    units = act_ref.shape[1]
    both = jnp.dot(h_ref[...], w_ref[...], preferred_element_type=f32)
    both_ref[...] = both
    gate = both[:, :units]
    act_ref[...] = (gate * jax.nn.sigmoid(gate) * both[:, units:]).astype(bf16)


def feed(h2, weight, tile=256):
    tokens, width = h2.shape
    units = weight.shape[1] // 2
    return pl.pallas_call(
        feed_kernel,
        grid=(tokens // tile,),
        in_specs=[
            pl.BlockSpec((tile, width), lambda i: (i, 0)),
            pl.BlockSpec((width, 2 * units), lambda i: (0, 0)),
        ],
        out_specs=[
            pl.BlockSpec((tile, 2 * units), lambda i: (i, 0)),
            pl.BlockSpec((tile, units), lambda i: (i, 0)),
        ],
        out_shape=[
            jax.ShapeDtypeStruct((tokens, 2 * units), f32),
            jax.ShapeDtypeStruct((tokens, units), bf16),
        ],
        cost_estimate=pl.CostEstimate(
            flops=4 * tokens * width * units, transcendentals=tokens * units,
            bytes_accessed=2 * tokens * width + 4 * width * units + 10 * tokens * units),
        name="feed",
    )(h2, weight)


def feed_back_kernel(d_ref, w_ref, both_ref, out_ref):
    units = w_ref.shape[0]
    d_act = lax.dot_general(d_ref[...], w_ref[...], (((1,), (1,)), ((), ())),
                            preferred_element_type=f32)
    gate, upward = both_ref[:, :units], both_ref[:, units:]
    sigmoid = jax.nn.sigmoid(gate)
    out_ref[:, :units] = (
        d_act * upward * sigmoid * (1.0 + gate * (1.0 - sigmoid))
    ).astype(bf16)
    out_ref[:, units:] = (d_act * gate * sigmoid).astype(bf16)


def feed_back(d_branch, weight, both, tile=256):
    tokens, width = d_branch.shape
    units = weight.shape[0]
    return pl.pallas_call(
        feed_back_kernel,
        grid=(tokens // tile,),
        in_specs=[
            pl.BlockSpec((tile, width), lambda i: (i, 0)),
            pl.BlockSpec((units, width), lambda i: (0, 0)),
            pl.BlockSpec((tile, 2 * units), lambda i: (i, 0)),
        ],
        out_specs=pl.BlockSpec((tile, 2 * units), lambda i: (i, 0)),
        out_shape=jax.ShapeDtypeStruct((tokens, 2 * units), bf16),
        cost_estimate=pl.CostEstimate(
            flops=2 * tokens * width * units, transcendentals=tokens * units,
            bytes_accessed=2 * tokens * width + 2 * width * units + 12 * tokens * units),
        name="feed_back",
    )(d_branch, weight, both)


def finish_kernel(s_ref, *refs, n, steps, outs, place):
    ins, out_refs = refs[:-outs], refs[-outs:]
    for stream in range(len(ins) // n):
        group = ins[stream * n : (stream + 1) * n]

        @pl.when(pl.program_id(0) // steps == stream)
        def _():
            got = [item[...] for item in group]
            place([choose(s_ref[0], [got[i ^ k] for i in range(n)]) for k in range(n)], out_refs)


def finish(s, streams, widths, place, tile, count=None):
    n = len(streams[0])
    columns = streams[0][0].shape[1]
    count = count or streams[0][0].shape[0]
    steps = count // tile
    rows = count * len(streams)
    specs = []
    for index in range(len(streams)):
        spec = pl.BlockSpec(
            (tile, columns),
            lambda i, s, index=index: (jnp.clip(i - index * steps, 0, steps - 1), 0),
        )
        specs += [spec] * n
    return pl.pallas_call(
        functools.partial(
            finish_kernel, n=n, steps=steps, outs=len(widths), place=place
        ),
        grid_spec=pltpu.PrefetchScalarGridSpec(
            num_scalar_prefetch=1,
            grid=(steps * len(streams),),
            in_specs=specs,
            out_specs=[pl.BlockSpec((tile, width), lambda i, s: (i, 0)) for width in widths],
        ),
        out_shape=[jax.ShapeDtypeStruct((rows, width), f32) for width in widths],
        cost_estimate=pl.CostEstimate(
            flops=0, bytes_accessed=6 * rows * sum(widths), transcendentals=0),
    )(s.reshape(1), *[item for group in streams for item in group])


def place_columns(parts, pieces, outs):
    width = pieces[0].shape[1] // parts
    for c in range(parts):
        for k, item in enumerate(pieces):
            first = (c * len(pieces) + k) * width
            outs[0][:, first : first + width] = item[:, c * width : (c + 1) * width].astype(f32)


def place_units(shards, pieces, outs):
    units = pieces[0].shape[1] // 2
    piece = units // shards
    wide = piece * len(pieces)
    pieces = [item.astype(f32) for item in pieces]
    for base, out in zip((0, units), outs):
        for i in range(shards):
            first = base + i * piece
            out[:, i * wide : (i + 1) * wide] = jnp.concatenate(
                [item[:, first : first + piece] for item in pieces], axis=1
            )


def rope_tables(tokens):
    lane = jnp.arange(2 * HD, dtype=jnp.int32)[None, :] % HD
    turned = lane < ROT
    freq = ROPE_BASE ** (-((lane % HALF).astype(f32) * 2.0) / ROT)
    angle = jnp.arange(tokens, dtype=jnp.int32)[:, None].astype(f32) * freq
    sine = jnp.sin(angle)
    return (
        jnp.where(turned, jnp.cos(angle), 1.0),
        jnp.where(lane < HALF, -sine, 0.0),
        jnp.where(turned & (lane >= HALF), sine, 0.0),
    )


def body(
    hidden_in,
    cotangent,
    block_table,
    first_gain,
    first_bias,
    qkv_weight,
    qkv_bias,
    out_weight,
    second_gain,
    second_bias,
    gate_weight,
    up_weight,
    down_weight,
    *,
    n,
    fs,
):
    s = lax.axis_index("seq")
    inputs = hidden_in[0].astype(f32)
    own, width = inputs.shape
    part = width // n
    rows = width // fs
    ffn = gate_weight.shape[1]
    units = ffn // n
    shard = ffn // fs
    piece = units // fs
    tokens = n * own
    order = [s ^ j for j in range(n)]

    blocks = jnp.concatenate(
        [lax.dynamic_slice_in_dim(block_table, order[j], 1, 0)[0] for j in range(n)]
    )
    ids = jnp.arange(2 * n, dtype=jnp.int32)
    slot = jnp.sum(jnp.where(blocks[None, :] == ids[:, None], ids[None, :], 0), axis=1)
    tables = rope_tables(tokens)

    d_own = cotangent[0]
    d_branch = jnp.concatenate(spread_seq(d_own, n), axis=0)

    def gather_fsdp(value):
        return lax.all_gather(value, "fsdp", axis=0, tiled=True)

    small = jnp.concatenate([first_gain, first_bias, second_gain, second_bias, qkv_bias])
    small = lax.all_gather(small, "fsdp", axis=0)
    vec = lambda i: small[:, i * rows : (i + 1) * rows].reshape(width).astype(f32)
    gain_one, bias_one, gain_two, bias_two = (vec(i) for i in range(4))
    bias_qkv = small[:, 4 * rows :].reshape(3, width).astype(f32)

    qkv_part = choose(
        s,
        [
            jnp.concatenate(
                [
                    qkv_weight[:, c * width + i * part : c * width + (i + 1) * part]
                    for c in range(3)
                ],
                axis=1,
            )
            for i in range(n)
        ],
    )
    out_part = choose(s, [out_weight[:, i * part : (i + 1) * part] for i in range(n)])
    w_first = gather_fsdp(jnp.concatenate([qkv_part, out_part], axis=1))
    w_qkv = w_first[:, : 3 * part]

    normed_one, inverse_one = normalize(inputs)
    h1_own = (normed_one * gain_one + bias_one).astype(bf16)
    picked = jnp.arange(units, dtype=jnp.int32)
    picked = (picked // piece) * shard + s * piece + picked % piece
    picked = after(picked, h1_own)
    pick = (jnp.arange(ffn, dtype=jnp.int32)[:, None] == picked[None, :]).astype(bf16)
    gate_up = jnp.concatenate(
        [
            jnp.dot(gate_weight, pick, preferred_element_type=f32).astype(bf16),
            jnp.dot(up_weight, pick, preferred_element_type=f32).astype(bf16),
        ],
        axis=1,
    )
    w_gate_up = gather_fsdp(gate_up)
    w_down = gather_fsdp(choose(s, [down_weight[i * piece : (i + 1) * piece] for i in range(n)]))

    h1 = jnp.concatenate(gather_seq(h1_own, n), axis=0)
    core = lax.axis_index("fsdp") % 2
    half = width // 2
    w_out_half = choose(core, [w_first[:half, 3 * part :], w_first[half:, 3 * part :]])
    w_out_pieces = spread_seq(after(w_out_half, h1), n)
    bias_part = choose(s, [bias_qkv[:, i * part : (i + 1) * part] for i in range(n)])
    projected = jnp.dot(h1, w_qkv, preferred_element_type=f32)
    projected = projected + bias_part.reshape(3 * part)
    head_out, lse, query, key, value = attend(slot, projected, tables)

    def natural(pieces):
        return [choose(s, [pieces[i ^ k] for i in range(n)]) for k in range(n)]

    def to_columns(pieces):
        return jnp.concatenate(natural(pieces), axis=1)

    def column_parts(value):
        return natural([value[:, k * part : (k + 1) * part] for k in range(n)])

    mixed = to_columns(
        exchange_seq([head_out[j * own : (j + 1) * own] for j in range(n)], n)
    )
    w_out = to_columns(w_out_pieces)
    w_out = [w_out, lax.ppermute(w_out, "fsdp", [(i, i ^ 1) for i in range(fs)])]
    by_core = lambda a, b: [jnp.where(core == 0, a, b), jnp.where(core == 0, b, a)]
    mixed_first, mixed_second = by_core(mixed[:, :half], mixed[:, half:])
    residual = (
        inputs
        + jnp.dot(mixed_first, w_out[0], preferred_element_type=f32)
        + jnp.dot(mixed_second, w_out[1], preferred_element_type=f32)
    )

    normed_two, inverse_two = normalize(residual)
    h2 = jnp.concatenate(gather_seq((normed_two * gain_two + bias_two).astype(bf16), n), axis=0)
    gate_up, activated = feed(h2, w_gate_up)

    across = (((1,), (1,)), ((), ()))
    down = (((0,), (0,)), ((), ()))
    dot = functools.partial(lax.dot_general, preferred_element_type=f32)

    def scatter_fsdp(value):
        return lax.psum_scatter(value, "fsdp", scatter_dimension=0, tiled=True)

    down_term = dot(activated, d_branch, down).astype(bf16)
    down_grad = scatter_fsdp(down_term)
    mixed_all = jnp.concatenate(spread_seq(after(mixed, h2), n), axis=0)
    branch = dot(after(activated, down_term), w_down, (((1,), (0,)), ((), ())))
    d_gate_up = feed_back(after(d_branch, branch), w_down, gate_up)
    branch = collect_seq([branch[j * own : (j + 1) * own] for j in range(n)], n)
    block_out = (residual + branch).astype(bf16)
    gate_up_term = dot(h2, d_gate_up, down).astype(bf16)
    gate_up_grad = scatter_fsdp(gate_up_term)
    d_h2 = dot(after(d_gate_up, gate_up_term), w_gate_up, across)
    d_h2 = scatter_seq([d_h2[j * own : (j + 1) * own] for j in range(n)], n)
    gain_two_grad = jnp.sum(d_h2 * normed_two, axis=0)
    bias_two_grad = jnp.sum(d_h2, axis=0)
    d_residual = d_own.astype(f32) + norm_back(d_h2, normed_two, inverse_two, gain_two)

    d_attended = d_residual.astype(bf16)
    d_mixed = by_core(*[dot(d_attended, item, across).astype(bf16) for item in w_out])
    d_mixed = jnp.concatenate(d_mixed, axis=1)
    d_mixed = jnp.concatenate(exchange_seq(column_parts(d_mixed), n), axis=0)
    d_projected = attend_back(
        slot, query, key, value, d_mixed, lse.transpose(0, 2, 1), tables
    )
    d_attended_part = exchange_seq(column_parts(after(d_attended, d_mixed)), n)
    d_attended_part = jnp.concatenate(d_attended_part, axis=0)
    down_pieces = spread_seq(after(down_grad, d_mixed), n)
    out_term = dot(mixed_all, d_attended_part, down).astype(bf16)
    qkv_term = dot(h1, d_projected, down).astype(bf16)
    qkv_grad = scatter_fsdp(qkv_term)
    qkv_bias_part = jnp.sum(d_projected.astype(f32), axis=0)
    d_h1 = dot(after(d_projected, qkv_term), w_qkv, across)
    d_h1 = scatter_seq([d_h1[j * own : (j + 1) * own] for j in range(n)], n)
    gain_one_grad = jnp.sum(d_h1 * normed_one, axis=0)
    bias_one_grad = jnp.sum(d_h1, axis=0)
    input_grad = (
        d_residual + norm_back(d_h1, normed_one, inverse_one, gain_one)
    ).astype(bf16)

    bias_all = jnp.concatenate(
        [jnp.where(s == i, qkv_bias_part.reshape(3, part), 0.0) for i in range(n)], axis=1
    )
    small = [
        gain_one_grad.reshape(fs, rows),
        bias_one_grad.reshape(fs, rows),
        gain_two_grad.reshape(fs, rows),
        bias_two_grad.reshape(fs, rows),
        bias_all.reshape(fs, 3 * rows),
    ]
    extra = -(-7 * rows // part)
    extra += -extra % 16
    small.append(jnp.zeros((fs, extra * part - 7 * rows), f32))
    small = jnp.concatenate(small, axis=1).astype(bf16).reshape(fs, extra, part)
    out_term = jnp.concatenate([out_term.reshape(fs, rows, part), small], axis=1)
    out_grad = scatter_fsdp(out_term.reshape(fs * (rows + extra), part))

    down_total = jnp.stack(natural(down_pieces)).reshape(shard, width).astype(f32)
    gate_up_pieces = gather_streams(after(gate_up_grad, qkv_term), n, d_h1)
    gate_total, up_total = finish(
        s, gate_up_pieces, (ffn, ffn),
        functools.partial(place_units, fs), min(64, rows // 2))
    qkv_pieces = gather_streams(after(qkv_grad, gate_up_pieces[0][n - 1]), n)
    (qkv_total,) = finish(
        s, qkv_pieces, (3 * width,),
        functools.partial(place_columns, 3), min(64, rows // 2))
    out_pieces = spread_seq(after(out_grad, qkv_pieces[1][n - 1]), n)
    (out_total,) = finish(
        s, [out_pieces], (width,),
        functools.partial(place_columns, 1), rows, rows)
    sums = sum(got[rows:].astype(f32) for got in out_pieces).reshape(extra * part)
    return (
        block_out[None],
        input_grad[None],
        sums[:rows],
        sums[rows : 2 * rows],
        qkv_total,
        sums[4 * rows : 7 * rows],
        out_total,
        sums[2 * rows : 3 * rows],
        sums[3 * rows : 4 * rows],
        gate_total,
        up_total,
        down_total,
    )


def solution(mesh):
    split = P("fsdp", None)
    act = P("fsdp", "seq", None)
    vec = P("fsdp")
    return jax.shard_map(
        functools.partial(body, n=mesh.shape["seq"], fs=mesh.shape["fsdp"]),
        mesh=mesh,
        in_specs=(act, act, P(), vec, vec, split, vec, split, vec, vec, split, split, split),
        out_specs=(act, act, vec, vec, split, vec, split, vec, vec, split, split, split),
        check_vma=False,
    )
```

```python
import functools

import jax
import jax.numpy as jnp
from jax import lax
from jax.experimental import pallas as pl
from jax.experimental.pallas import tpu as pltpu
from jax.sharding import PartitionSpec as P


HD = 64
ROT = HD // 4
HALF = ROT // 2
EPS = 1e-05
ROPE_BASE = 10000.0
NEG = -1e30
SCALE = float(HD) ** -0.5
f32 = jnp.float32
bf16 = jnp.bfloat16


def normalize(values):
    centred = values - jnp.mean(values, axis=-1, keepdims=True)
    inverse = lax.rsqrt(jnp.mean(centred * centred, axis=-1, keepdims=True) + EPS)
    return (centred * inverse, inverse)


def norm_back(d_normed, normed, inverse, gain):
    scaled = d_normed * gain
    return inverse * (
        scaled
        - jnp.mean(scaled, axis=-1, keepdims=True)
        - normed * jnp.mean(scaled * normed, axis=-1, keepdims=True)
    )


def swap(value, mask, n):
    return lax.ppermute(value, "seq", [(i, i ^ mask) for i in range(n)])


def after(value, first):
    return lax.optimization_barrier((value, first))[0]


def halves(count):
    middle = (count // 2 + 8) // 16 * 16
    return ((0, middle), (middle, count))


def gather_streams(value, n, second=None):
    bits = n.bit_length() - 1
    streams = [{0: value[first:last]} for first, last in halves(value.shape[0])]
    for step in range(bits):
        for index, have in enumerate(streams):
            mask = 1 << ((index + step) % bits)
            items = have
            if step:
                last = list(have)[-1]
                items = {k: after(v, have[last]) for k, v in have.items() if k != last}
                items[last] = have[last]
                if second is not None:
                    items = {k: after(v, second) for k, v in items.items()}
            have.update({key ^ mask: swap(item, mask, n) for key, item in items.items()})
    return [[have[j] for j in range(n)] for have in streams]


def gather_seq(value, n, second=None):
    streams = gather_streams(value, n, second)
    return [jnp.concatenate(pair, axis=0) for pair in zip(*streams)]


def exchange_seq(pieces, n):
    return [pieces[0]] + [swap(pieces[j], j, n) for j in range(1, n)]


def spread_seq(value, n):
    return exchange_seq([value] * n, n)


def choose(index, options):
    out = options[0]
    for i, option in enumerate(options[1:], 1):
        out = jnp.where(index == i, option, out)
    return out


def flip(s, mask, n):
    out = 0
    bit = 1
    while bit < n:
        out += bit * ((s // bit + mask // bit) % 2)
        bit *= 2
    return out


def greet(partners):
    barrier = pltpu.get_barrier_semaphore()
    for partner in partners:
        pl.semaphore_signal(
            barrier, inc=1, device_id={"seq": partner}, device_id_type=pl.DeviceIdType.MESH
        )
    pl.semaphore_wait(barrier, len(partners))


def dot_scatter_kernel(
    a_ref, w_ref, *refs, n, tile, ride
):
    if ride:
        x_ref, out_ref, x_out_ref, *refs, x_sent, x_came, x_local = refs
    else:
        out_ref, *refs = refs
    w_buf, acc, out_buf, in_buf, sent, came, local = refs
    bits = n.bit_length() - 1
    s = lax.axis_index("seq")
    rows = a_ref.shape[0] // n
    width = w_ref.shape[0]
    cut = halves(rows)

    def load(i):
        span = pl.ds(pl.multiple_of(i * tile, tile), tile)
        return pltpu.make_async_copy(
            w_ref.at[span, pl.ds(0, a_ref.shape[1])], w_buf.at[span, :], local.at[i])

    for i in range(width // tile):
        load(i).start()
    copies = {}
    if ride:
        greet([flip(s, j, n) for j in range(1, n)])
        part = x_out_ref.shape[1]
        for j in range(1, n):
            partner = flip(s, j, n)
            copy = pltpu.make_async_remote_copy(
                src_ref=x_ref.at[:, pl.ds(pl.multiple_of(partner * part, part), part)],
                dst_ref=x_out_ref.at[pl.ds(j * rows, rows), :],
                send_sem=x_sent.at[j], recv_sem=x_came.at[j],
                device_id={"seq": partner}, device_id_type=pl.DeviceIdType.MESH,
            )
            copy.start()
            copies["ride", j] = copy
        keep = pltpu.make_async_copy(
            x_ref.at[:, pl.ds(pl.multiple_of(s * part, part), part)],
            x_out_ref.at[pl.ds(0, rows), :], x_local)
        keep.start()
        keep.wait()
    else:
        greet([flip(s, 1 << bit, n) for bit in range(bits)])

    def mask_of(stream, step):
        return 1 << ((stream + bits - 1 - step) % bits)

    def ship(stream, key, mask):
        span = pl.ds(cut[stream][0], cut[stream][1] - cut[stream][0])
        out_buf[key, span, :] = acc[key, span, :].astype(bf16)
        copy = pltpu.make_async_remote_copy(
            src_ref=out_buf.at[key, span, :],
            dst_ref=in_buf.at[key, span, :],
            send_sem=sent.at[stream, key],
            recv_sem=came.at[stream, key],
            device_id={"seq": flip(s, mask, n)},
            device_id_type=pl.DeviceIdType.MESH,
        )
        copy.start()
        copies[stream, key] = copy

    for key in sorted(range(n), key=lambda k: (-bin(k).count("1"), -k)):

        def columns(i, _, key=key):
            span = pl.ds(pl.multiple_of(i * tile, tile), tile)
            if key == n - 1:
                load(i).wait()
            acc[key, :, span] = lax.dot_general(
                a_ref[pl.ds(key * rows, rows), :], w_buf[span, :],
                (((1,), (1,)), ((), ())), preferred_element_type=f32)
            return 0

        lax.fori_loop(0, width // tile, columns, 0)
        for stream in range(2):
            mask = mask_of(stream, 0)
            if key & mask:
                ship(stream, key, mask)
    have = [list(range(n)), list(range(n))]
    for step in range(bits):
        for stream in range(2):
            mask = mask_of(stream, step)
            span = pl.ds(cut[stream][0], cut[stream][1] - cut[stream][0])
            kept = [key for key in have[stream] if not key & mask]
            if step:
                for key in have[stream]:
                    if key & mask:
                        ship(stream, key, mask)
            have[stream] = kept
        for stream in range(2):
            mask = mask_of(stream, step)
            span = pl.ds(cut[stream][0], cut[stream][1] - cut[stream][0])
            for key in have[stream]:
                copies[stream, key ^ mask].wait_recv()
                total = acc[key, span, :] + in_buf[key ^ mask, span, :].astype(f32)
                if step == bits - 1:
                    out_ref[span, :] = total
                else:
                    acc[key, span, :] = total
    for key, copy in copies.items():
        copy.wait_send()
        if key[0] == "ride":
            copy.wait_recv()


def dot_scatter(a, weight, n, collective_id, ride=None, tile=512):
    rows, depth = a.shape
    width = weight.shape[0]
    own = rows // n
    block = lambda shape: pl.BlockSpec(shape, lambda i: (0, 0))
    return pl.pallas_call(
        functools.partial(dot_scatter_kernel, n=n, tile=tile, ride=ride is not None),
        grid=(1,),
        in_specs=[block((rows, depth)), pl.BlockSpec(memory_space=pl.ANY)]
        + ([] if ride is None else [block(ride.shape)]),
        out_specs=[block((own, width))]
        + ([] if ride is None else [block((rows, ride.shape[1] // n))]),
        out_shape=[jax.ShapeDtypeStruct((own, width), f32)]
        + ([] if ride is None else [jax.ShapeDtypeStruct((rows, ride.shape[1] // n), bf16)]),
        scratch_shapes=[
            pltpu.VMEM((width, depth), bf16),
            pltpu.VMEM((n, own, width), f32),
            pltpu.VMEM((n, own, width), bf16),
            pltpu.VMEM((n, own, width), bf16),
            pltpu.SemaphoreType.DMA((2, n)),
            pltpu.SemaphoreType.DMA((2, n)),
            pltpu.SemaphoreType.DMA((width // tile,)),
        ]
        + ([] if ride is None else [
            pltpu.SemaphoreType.DMA((n,)),
            pltpu.SemaphoreType.DMA((n,)),
            pltpu.SemaphoreType.DMA(()),
        ]),
        compiler_params=pltpu.CompilerParams(
            collective_id=collective_id, has_side_effects=True),
        cost_estimate=pl.CostEstimate(
            flops=2 * rows * depth * width, transcendentals=0,
            bytes_accessed=40 * rows * width),
    )(a, weight, *([] if ride is None else [ride]))


def pair_dot_kernel(
    a_ref, b_ref, out_ref, mine, other, out_buf, in_buf, sent, came, local, *, shards, tile
):
    me = lax.axis_index("fsdp")
    core = me % 2
    partner = me + 1 - 2 * core
    block = a_ref.shape[0] // shards
    loads = []
    for side, (to, parity) in enumerate(((other, 1 - core), (mine, core))):
        for z in range(shards // 2):
            first = pl.multiple_of((2 * z + parity) * block, block)
            load = pltpu.make_async_copy(
                a_ref.at[pl.ds(first, block), :], to.at[pl.ds(z * block, block), :],
                local.at[side, z])
            load.start()
            loads.append(load)
    barrier = pltpu.get_barrier_semaphore()
    pl.semaphore_signal(
        barrier, inc=1, device_id={"fsdp": partner}, device_id_type=pl.DeviceIdType.MESH
    )
    pl.semaphore_wait(barrier, 1)
    for load in loads:
        load.wait()
    steps = b_ref.shape[1] // tile
    edges = (0, (steps + 1) // 2, steps)
    copies = []
    for part in range(2):

        def keep(i, _):
            cols = pl.ds(pl.multiple_of(i * tile, tile), tile)
            out_buf[:, cols] = jnp.dot(
                other[...], b_ref[:, cols], preferred_element_type=f32).astype(bf16)
            return 0

        lax.fori_loop(edges[part], edges[part + 1], keep, 0)
        span = pl.ds(edges[part] * tile, (edges[part + 1] - edges[part]) * tile)
        copy = pltpu.make_async_remote_copy(
            src_ref=out_buf.at[:, span], dst_ref=in_buf.at[:, span],
            send_sem=sent.at[part], recv_sem=came.at[part],
            device_id={"fsdp": partner}, device_id_type=pl.DeviceIdType.MESH,
        )
        copy.start()
        copies.append(copy)
    for part in range(2):
        copies[part].wait_recv()

        def add(i, _):
            cols = pl.ds(pl.multiple_of(i * tile, tile), tile)
            total = jnp.dot(mine[...], b_ref[:, cols], preferred_element_type=f32)
            out_ref[:, cols] = (total + in_buf[:, cols].astype(f32)).astype(bf16)
            return 0

        lax.fori_loop(edges[part], edges[part + 1], add, 0)
    for copy in copies:
        copy.wait_send()


def pair_dot(turned, b, shards, collective_id):
    rows, tokens = turned.shape
    rows //= 2
    width = b.shape[1]
    tile = 256 if width % 256 == 0 else 128
    whole = lambda shape: pl.BlockSpec(shape, lambda i: (0, 0))
    return pl.pallas_call(
        functools.partial(pair_dot_kernel, shards=shards, tile=tile),
        grid=(1,),
        in_specs=[pl.BlockSpec(memory_space=pl.ANY), whole((tokens, width))],
        out_specs=whole((rows, width)),
        out_shape=jax.ShapeDtypeStruct((rows, width), bf16),
        scratch_shapes=[
            pltpu.VMEM((rows, tokens), bf16),
            pltpu.VMEM((rows, tokens), bf16),
            pltpu.VMEM((rows, width), bf16),
            pltpu.VMEM((rows, width), bf16),
            pltpu.SemaphoreType.DMA((2,)),
            pltpu.SemaphoreType.DMA((2,)),
            pltpu.SemaphoreType.DMA((2, shards // 2)),
        ],
        compiler_params=pltpu.CompilerParams(
            collective_id=collective_id, has_side_effects=True),
        cost_estimate=pl.CostEstimate(
            flops=4 * tokens * rows * width, transcendentals=0,
            bytes_accessed=10 * tokens * width),
    )(turned, b)


def column_of(group, core, n, part):
    half = n // 2
    return pl.multiple_of(((group // half + core) % 2) * half * part + (group % half) * part, part)


def exchange_kernel(x_ref, out_ref, sent, came, local, *, n, part, to_columns):
    s = lax.axis_index("seq")
    core = lax.axis_index("fsdp") % 2
    rows = (x_ref if not to_columns else out_ref).shape[0]
    partners = [flip(s, j, n) for j in range(1, n)]
    greet(partners)
    copies = []
    for j in list(range(1, n)):
        partner = partners[j - 1]
        if to_columns:
            src = x_ref.at[pl.ds(j * rows, rows), :]
            dst = out_ref.at[:, pl.ds(column_of(s, core, n, part), part)]
        else:
            src = x_ref.at[:, pl.ds(column_of(partner, core, n, part), part)]
            dst = out_ref.at[pl.ds(j * rows, rows), :]
        copy = pltpu.make_async_remote_copy(
            src_ref=src, dst_ref=dst, send_sem=sent.at[j], recv_sem=came.at[j],
            device_id={"seq": partner}, device_id_type=pl.DeviceIdType.MESH,
        )
        copy.start()
        copies.append(copy)
    own = pl.ds(column_of(s, core, n, part), part)
    if to_columns:
        keep = pltpu.make_async_copy(x_ref.at[pl.ds(0, rows), :], out_ref.at[:, own], local)
    else:
        keep = pltpu.make_async_copy(x_ref.at[:, own], out_ref.at[pl.ds(0, rows), :], local)
    keep.start()
    keep.wait()
    for copy in copies:
        copy.wait()


def exchange(x, n, part, to_columns, collective_id):
    rows, width = x.shape
    shape = (rows // n, n * part) if to_columns else (rows * n, part)
    return pl.pallas_call(
        functools.partial(exchange_kernel, n=n, part=part, to_columns=to_columns),
        in_specs=[pl.BlockSpec(memory_space=pltpu.VMEM)],
        out_specs=pl.BlockSpec(memory_space=pltpu.VMEM),
        out_shape=jax.ShapeDtypeStruct(shape, x.dtype),
        scratch_shapes=[
            pltpu.SemaphoreType.DMA((n,)),
            pltpu.SemaphoreType.DMA((n,)),
            pltpu.SemaphoreType.DMA(()),
        ],
        compiler_params=pltpu.CompilerParams(
            collective_id=collective_id, has_side_effects=True),
        cost_estimate=pl.CostEstimate(
            flops=0, transcendentals=0, bytes_accessed=30 * rows * width),
    )(x)


def turn(tensor, cosine, left, right, sign):
    back = pltpu.roll(tensor, 2 * HD - HALF, 1)
    ahead = pltpu.roll(tensor, HALF, 1)
    return tensor * cosine + sign * (back * left + ahead * right)


def attend_kernel(slot_ref, q_ref, k_ref, v_ref, cos_ref, left_ref, right_ref,
                  o_ref, lse_ref, qo_ref, ko_ref, vo_ref, tile):
    tokens = q_ref.shape[0]
    slots = slot_ref.shape[0]
    blk = tokens // slots
    for p in range(slots):
        rows = pl.ds(pl.multiple_of(slot_ref[p] * blk, blk), blk)
        own = pl.ds(p * blk, blk)
        cosine, left, right = cos_ref[own, :], left_ref[own, :], right_ref[own, :]
        qo_ref[own, :] = turn(q_ref[rows, :], cosine, left, right, 1.0).astype(bf16)
        ko_ref[own, :] = turn(k_ref[rows, :], cosine, left, right, 1.0).astype(bf16)
        vo_ref[own, :] = v_ref[rows, :].astype(bf16)
    mask = lax.broadcasted_iota(jnp.int32, (tile, tile), 1) <= lax.broadcasted_iota(
        jnp.int32, (tile, tile), 0
    )
    for t in range(tokens // tile):
        own = pl.ds(t * tile, tile)
        outs, stats = [], []
        for h in range(2):
            lanes = pl.ds(h * HD, HD)
            query = qo_ref[own, lanes]
            end = (t + 1) * tile
            scores = lax.dot_general(
                query, ko_ref[pl.ds(0, end), lanes], (((1,), (1,)), ((), ())),
                preferred_element_type=f32) * SCALE
            diag = jnp.where(mask, scores[:, t * tile :], NEG)
            scores = jnp.concatenate([scores[:, : t * tile], diag], axis=1) if t else diag
            peak = jnp.max(scores, axis=1, keepdims=True)
            weights = jnp.exp(scores - peak)
            total = jnp.sum(weights, axis=1, keepdims=True)
            weights = (weights * (1.0 / total)).astype(bf16)
            outs.append(jnp.dot(weights, vo_ref[pl.ds(0, end), lanes],
                                preferred_element_type=f32))
            stats.append(peak + jnp.log(total))
        out = jnp.concatenate(outs, axis=1).astype(bf16)
        lse_ref[0, own, :] = jnp.concatenate(stats, axis=1)
        for part in range(tile // blk):
            rows = pl.ds(pl.multiple_of(slot_ref[t * (tile // blk) + part] * blk, blk), blk)
            o_ref[rows, :] = out[part * blk : (part + 1) * blk]


def attend(slot, projected, tables, tile=256):
    tokens, width = projected.shape
    width //= 3
    groups = width // (2 * HD)
    lanes = 2 * HD
    col = lambda base: pl.BlockSpec((tokens, lanes), lambda i, s: (0, base + i))
    table = pl.BlockSpec((tokens, lanes), lambda i, s: (0, 0))
    return pl.pallas_call(
        functools.partial(attend_kernel, tile=tile),
        grid_spec=pltpu.PrefetchScalarGridSpec(
            num_scalar_prefetch=1,
            grid=(groups,),
            in_specs=[col(0), col(groups), col(2 * groups), table, table, table],
            out_specs=[col(0), pl.BlockSpec((1, tokens, 2), lambda i, s: (i, 0, 0)),
                       col(0), col(0), col(0)],
        ),
        out_shape=[
            jax.ShapeDtypeStruct((tokens, width), bf16),
            jax.ShapeDtypeStruct((groups, tokens, 2), f32),
            jax.ShapeDtypeStruct((tokens, width), bf16),
            jax.ShapeDtypeStruct((tokens, width), bf16),
            jax.ShapeDtypeStruct((tokens, width), bf16),
        ],
        cost_estimate=pl.CostEstimate(
            flops=4 * tokens * tokens * width, bytes_accessed=24 * tokens * width,
            transcendentals=tokens * tokens * 2 * groups),
        name="attend",
    )(slot, projected, projected, projected, *tables)


def attend_back_kernel(slot_ref, q_ref, k_ref, v_ref, d_ref, lse_ref,
                       cos_ref, left_ref, right_ref, g_ref,
                       d_pos, dq_acc, dk_acc, dv_acc, tile):
    tokens = q_ref.shape[0]
    slots = slot_ref.shape[0]
    blk = tokens // slots
    width = g_ref.shape[1] // 3
    group = pl.program_id(0)
    for p in range(slots):
        rows = pl.ds(pl.multiple_of(slot_ref[p] * blk, blk), blk)
        d_pos[pl.ds(p * blk, blk), :] = d_ref[rows, :]
    dk_acc[...] = jnp.zeros_like(dk_acc)
    dv_acc[...] = jnp.zeros_like(dv_acc)
    mask = lax.broadcasted_iota(jnp.int32, (tile, tile), 0) <= lax.broadcasted_iota(
        jnp.int32, (tile, tile), 1
    )
    for t in range(tokens // tile):
        own = pl.ds(t * tile, tile)
        past = pl.ds(0, (t + 1) * tile)
        grads = []
        keys_grad, values_grad = [], []
        for h in range(2):
            lanes = pl.ds(h * HD, HD)
            query, keys = q_ref[own, lanes], k_ref[past, lanes]
            d_out = d_pos[own, lanes]
            scores = lax.dot_general(keys, query, (((1,), (1,)), ((), ())),
                                     preferred_element_type=f32) * SCALE
            diag = jnp.where(mask, scores[t * tile :], NEG)
            scores = jnp.concatenate([scores[: t * tile], diag], axis=0) if t else diag
            probs = jnp.exp(scores - lse_ref[0, pl.ds(h, 1), own])
            d_probs = lax.dot_general(v_ref[past, lanes], d_out, (((1,), (1,)), ((), ())),
                                      preferred_element_type=f32)
            delta = jnp.sum(d_probs * probs, axis=0, keepdims=True)
            d_scores = (probs * (d_probs - delta)).astype(bf16)
            values_grad.append(jnp.dot(probs.astype(bf16), d_out, preferred_element_type=f32))
            keys_grad.append(jnp.dot(d_scores, query, preferred_element_type=f32))
            grads.append(lax.dot_general(d_scores, keys, (((0,), (0,)), ((), ())),
                                         preferred_element_type=f32))
        dk_acc[past, :] += jnp.concatenate(keys_grad, axis=1)
        dv_acc[past, :] += jnp.concatenate(values_grad, axis=1)
        dq_acc[own, :] = jnp.concatenate(grads, axis=1)
    lanes = 2 * HD
    for p in range(slots):
        rows = pl.ds(pl.multiple_of(slot_ref[p] * blk, blk), blk)
        own = pl.ds(p * blk, blk)
        cosine, left, right = cos_ref[own, :], left_ref[own, :], right_ref[own, :]
        first = pl.multiple_of(group * lanes, lanes)
        g_ref[rows, pl.ds(first, lanes)] = turn(
            dq_acc[own, :] * SCALE, cosine, left, right, -1.0).astype(bf16)
        g_ref[rows, pl.ds(width + first, lanes)] = turn(
            dk_acc[own, :] * SCALE, cosine, left, right, -1.0).astype(bf16)
        g_ref[rows, pl.ds(2 * width + first, lanes)] = dv_acc[own, :].astype(bf16)


def attend_back(slot, query, key, value, d_mixed, lse, tables, tile=256):
    tokens, width = query.shape
    groups = width // (2 * HD)
    lanes = 2 * HD
    col = pl.BlockSpec((tokens, lanes), lambda i, s: (0, i))
    table = pl.BlockSpec((tokens, lanes), lambda i, s: (0, 0))
    return pl.pallas_call(
        functools.partial(attend_back_kernel, tile=tile),
        grid_spec=pltpu.PrefetchScalarGridSpec(
            num_scalar_prefetch=1,
            grid=(groups,),
            in_specs=[col, col, col, col,
                      pl.BlockSpec((1, 2, tokens), lambda i, s: (i, 0, 0)),
                      table, table, table],
            out_specs=pl.BlockSpec((tokens, 3 * width), lambda i, s: (0, 0)),
            scratch_shapes=[pltpu.VMEM((tokens, lanes), bf16)]
            + [pltpu.VMEM((tokens, lanes), f32)] * 3,
        ),
        out_shape=jax.ShapeDtypeStruct((tokens, 3 * width), bf16),
        cost_estimate=pl.CostEstimate(
            flops=10 * tokens * tokens * width, bytes_accessed=16 * tokens * width,
            transcendentals=tokens * tokens * 2 * groups),
        name="attend_back",
    )(slot, query, key, value, d_mixed, lse, *tables)


def project_kernel(h_ref, w_ref, bias_ref, out_ref, turned_ref):
    out_ref[...] = (
        jnp.dot(h_ref[...], w_ref[...], preferred_element_type=f32) + bias_ref[...]
    )
    turned_ref[...] = jnp.transpose(h_ref[...])


def project(h1, weight, bias, tile=256):
    tokens, width = h1.shape
    columns = bias.shape[1]
    return pl.pallas_call(
        project_kernel,
        grid=(tokens // tile,),
        in_specs=[
            pl.BlockSpec((tile, width), lambda i: (i, 0)),
            pl.BlockSpec((width, columns), lambda i: (0, 0)),
            pl.BlockSpec((1, columns), lambda i: (0, 0)),
        ],
        out_specs=[
            pl.BlockSpec((tile, columns), lambda i: (i, 0)),
            pl.BlockSpec((width, tile), lambda i: (0, i)),
        ],
        out_shape=[
            jax.ShapeDtypeStruct((tokens, columns), f32),
            jax.ShapeDtypeStruct((width, tokens), bf16),
        ],
        cost_estimate=pl.CostEstimate(
            flops=2 * tokens * width * columns, transcendentals=0,
            bytes_accessed=4 * tokens * width + 2 * width * columns + 4 * tokens * columns),
        name="project",
    )(h1, weight, bias)


def feed_kernel(h_ref, w_ref, both_ref, act_ref, turned_ref):
    units = act_ref.shape[1]
    both = jnp.dot(h_ref[...], w_ref[...], preferred_element_type=f32)
    both_ref[...] = both
    turned_ref[...] = jnp.transpose(h_ref[...])
    gate = both[:, :units]
    act_ref[...] = (gate * jax.nn.sigmoid(gate) * both[:, units:]).astype(bf16)


def feed(h2, weight, tile=256):
    tokens, width = h2.shape
    units = weight.shape[1] // 2
    return pl.pallas_call(
        feed_kernel,
        grid=(tokens // tile,),
        in_specs=[
            pl.BlockSpec((tile, width), lambda i: (i, 0)),
            pl.BlockSpec((width, 2 * units), lambda i: (0, 0)),
        ],
        out_specs=[
            pl.BlockSpec((tile, 2 * units), lambda i: (i, 0)),
            pl.BlockSpec((tile, units), lambda i: (i, 0)),
            pl.BlockSpec((width, tile), lambda i: (0, i)),
        ],
        out_shape=[
            jax.ShapeDtypeStruct((tokens, 2 * units), f32),
            jax.ShapeDtypeStruct((tokens, units), bf16),
            jax.ShapeDtypeStruct((width, tokens), bf16),
        ],
        cost_estimate=pl.CostEstimate(
            flops=4 * tokens * width * units, transcendentals=tokens * units,
            bytes_accessed=4 * tokens * width + 4 * width * units + 10 * tokens * units),
        name="feed",
    )(h2, weight)


def feed_back_kernel(d_ref, w_ref, both_ref, out_ref):
    units = w_ref.shape[0]
    d_act = lax.dot_general(d_ref[...], w_ref[...], (((1,), (1,)), ((), ())),
                            preferred_element_type=f32)
    gate, upward = both_ref[:, :units], both_ref[:, units:]
    sigmoid = jax.nn.sigmoid(gate)
    out_ref[:, :units] = (
        d_act * upward * sigmoid * (1.0 + gate * (1.0 - sigmoid))
    ).astype(bf16)
    out_ref[:, units:] = (d_act * gate * sigmoid).astype(bf16)


def feed_back(d_branch, weight, both, tile=256):
    tokens, width = d_branch.shape
    units = weight.shape[0]
    return pl.pallas_call(
        feed_back_kernel,
        grid=(tokens // tile,),
        in_specs=[
            pl.BlockSpec((tile, width), lambda i: (i, 0)),
            pl.BlockSpec((units, width), lambda i: (0, 0)),
            pl.BlockSpec((tile, 2 * units), lambda i: (i, 0)),
        ],
        out_specs=pl.BlockSpec((tile, 2 * units), lambda i: (i, 0)),
        out_shape=jax.ShapeDtypeStruct((tokens, 2 * units), bf16),
        cost_estimate=pl.CostEstimate(
            flops=2 * tokens * width * units, transcendentals=tokens * units,
            bytes_accessed=2 * tokens * width + 2 * width * units + 12 * tokens * units),
        name="feed_back",
    )(d_branch, weight, both)


def finish_kernel(s_ref, *refs, n, steps, outs, place):
    ins, out_refs = refs[:-outs], refs[-outs:]
    for stream in range(len(ins) // n):
        group = ins[stream * n : (stream + 1) * n]

        @pl.when(pl.program_id(0) // steps == stream)
        def _():
            got = [item[...] for item in group]
            place([choose(s_ref[0], [got[i ^ k] for i in range(n)]) for k in range(n)], out_refs)


def finish(s, streams, widths, place, tile, count=None):
    n = len(streams[0])
    columns = streams[0][0].shape[1]
    count = count or streams[0][0].shape[0]
    steps = count // tile
    rows = count * len(streams)
    specs = []
    for index in range(len(streams)):
        spec = pl.BlockSpec(
            (tile, columns),
            lambda i, s, index=index: (jnp.clip(i - index * steps, 0, steps - 1), 0),
        )
        specs += [spec] * n
    return pl.pallas_call(
        functools.partial(
            finish_kernel, n=n, steps=steps, outs=len(widths), place=place
        ),
        grid_spec=pltpu.PrefetchScalarGridSpec(
            num_scalar_prefetch=1,
            grid=(steps * len(streams),),
            in_specs=specs,
            out_specs=[pl.BlockSpec((tile, width), lambda i, s: (i, 0)) for width in widths],
        ),
        out_shape=[jax.ShapeDtypeStruct((rows, width), f32) for width in widths],
        cost_estimate=pl.CostEstimate(
            flops=0, bytes_accessed=6 * rows * sum(widths), transcendentals=0),
    )(s.reshape(1), *[item for group in streams for item in group])


def place_columns(parts, pieces, outs):
    width = pieces[0].shape[1] // parts
    for c in range(parts):
        for k, item in enumerate(pieces):
            first = (c * len(pieces) + k) * width
            outs[0][:, first : first + width] = item[:, c * width : (c + 1) * width].astype(f32)


def place_units(shards, pieces, outs):
    units = pieces[0].shape[1] // 2
    piece = units // shards
    wide = piece * len(pieces)
    pieces = [item.astype(f32) for item in pieces]
    for base, out in zip((0, units), outs):
        for i in range(shards):
            first = base + i * piece
            out[:, i * wide : (i + 1) * wide] = jnp.concatenate(
                [item[:, first : first + piece] for item in pieces], axis=1
            )


def rope_tables(tokens):
    lane = jnp.arange(2 * HD, dtype=jnp.int32)[None, :] % HD
    turned = lane < ROT
    freq = ROPE_BASE ** (-((lane % HALF).astype(f32) * 2.0) / ROT)
    angle = jnp.arange(tokens, dtype=jnp.int32)[:, None].astype(f32) * freq
    sine = jnp.sin(angle)
    return (
        jnp.where(turned, jnp.cos(angle), 1.0),
        jnp.where(lane < HALF, -sine, 0.0),
        jnp.where(turned & (lane >= HALF), sine, 0.0),
    )


def body(
    hidden_in,
    cotangent,
    block_table,
    first_gain,
    first_bias,
    qkv_weight,
    qkv_bias,
    out_weight,
    second_gain,
    second_bias,
    gate_weight,
    up_weight,
    down_weight,
    *,
    n,
    fs,
):
    s = lax.axis_index("seq")
    core = lax.axis_index("fsdp") % 2
    by_core = lambda a, b: [jnp.where(core == 0, a, b), jnp.where(core == 0, b, a)]

    inputs = hidden_in[0].astype(f32)
    own, width = inputs.shape
    part = width // n
    rows = width // fs
    ffn = gate_weight.shape[1]
    units = ffn // n
    shard = ffn // fs
    piece = units // fs
    tokens = n * own
    order = [s ^ j for j in range(n)]

    blocks = jnp.concatenate(
        [lax.dynamic_slice_in_dim(block_table, order[j], 1, 0)[0] for j in range(n)]
    )
    ids = jnp.arange(2 * n, dtype=jnp.int32)
    slot = jnp.sum(jnp.where(blocks[None, :] == ids[:, None], ids[None, :], 0), axis=1)
    tables = rope_tables(tokens)

    d_own = cotangent[0]
    d_branch = jnp.concatenate(spread_seq(d_own, n), axis=0)

    def gather_fsdp(value):
        return lax.all_gather(value, "fsdp", axis=0, tiled=True)

    small = jnp.concatenate([first_gain, first_bias, second_gain, second_bias, qkv_bias])
    small = lax.all_gather(small, "fsdp", axis=0)
    vec = lambda i: small[:, i * rows : (i + 1) * rows].reshape(width).astype(f32)
    gain_one, bias_one, gain_two, bias_two = (vec(i) for i in range(4))
    bias_qkv = small[:, 4 * rows :].reshape(3, width).astype(f32)

    qkv_part = choose(
        s,
        [
            jnp.concatenate(
                [
                    qkv_weight[:, c * width + i * part : c * width + (i + 1) * part]
                    for c in range(3)
                ],
                axis=1,
            )
            for i in range(n)
        ],
    )
    out_part = choose(s, [out_weight[:, i * part : (i + 1) * part] for i in range(n)])
    w_first = gather_fsdp(jnp.concatenate([qkv_part, out_part], axis=1))

    normed_one, inverse_one = normalize(inputs)
    h1_own = (normed_one * gain_one + bias_one).astype(bf16)
    picked = jnp.arange(units, dtype=jnp.int32)
    picked = (picked // piece) * shard + s * piece + picked % piece
    picked = after(picked, h1_own)
    pick = (jnp.arange(ffn, dtype=jnp.int32)[:, None] == picked[None, :]).astype(bf16)
    gate_up = jnp.concatenate(
        [
            jnp.dot(gate_weight, pick, preferred_element_type=f32).astype(bf16),
            jnp.dot(up_weight, pick, preferred_element_type=f32).astype(bf16),
        ],
        axis=1,
    )
    w_gate_up = gather_fsdp(gate_up)
    w_down = gather_fsdp(choose(s, [down_weight[i * piece : (i + 1) * piece] for i in range(n)]))

    h1 = jnp.concatenate(gather_seq(h1_own, n), axis=0)
    half = width // 2
    w_out_half = choose(core, [w_first[:half, 3 * part :], w_first[half:, 3 * part :]])
    w_out_pieces = spread_seq(after(w_out_half, h1), n)
    bias_part = choose(s, [bias_qkv[:, i * part : (i + 1) * part] for i in range(n)])
    projected, h1_turned = project(h1, w_first, bias_part.reshape(1, 3 * part))
    head_out, lse, query, key, value = attend(slot, projected, tables)

    def natural(pieces):
        return [choose(s, [pieces[i ^ k] for i in range(n)]) for k in range(n)]

    def to_columns(pieces):
        return jnp.concatenate(natural(pieces), axis=1)

    mixed = exchange(head_out, n, part, True, 1)
    w_out = to_columns(w_out_pieces)
    w_out = [w_out, lax.ppermute(w_out, "fsdp", [(i, i ^ 1) for i in range(fs)])]
    residual = (
        inputs
        + jnp.dot(mixed[:, :half], w_out[0], preferred_element_type=f32)
        + jnp.dot(mixed[:, half:], w_out[1], preferred_element_type=f32)
    )

    normed_two, inverse_two = normalize(residual)
    h2 = jnp.concatenate(gather_seq((normed_two * gain_two + bias_two).astype(bf16), n), axis=0)
    gate_up, activated, h2_turned = feed(h2, w_gate_up)

    across = (((1,), (1,)), ((), ()))
    down = (((0,), (0,)), ((), ()))
    dot = functools.partial(lax.dot_general, preferred_element_type=f32)

    def scatter_fsdp(value, groups=None):
        return lax.psum_scatter(
            value, "fsdp", scatter_dimension=0, tiled=True, axis_index_groups=groups)

    cores = [list(range(c, fs, 2)) for c in range(2)]

    def pair_sum(value):
        value = value.reshape(fs // 2, 2, -1, value.shape[1])
        mine, other = by_core(value[:, 0], value[:, 1])
        other = lax.ppermute(other, "fsdp", [(i, i ^ 1) for i in range(fs)])
        total = mine.astype(f32) + other.astype(f32)
        return total.astype(bf16).reshape(-1, value.shape[3])

    down_term = dot(activated, d_branch, down).astype(bf16)
    down_grad = scatter_fsdp(down_term)
    lse = lse.transpose(0, 2, 1)
    mixed_pieces = spread_seq(after(mixed, h2), n)
    branch = dot(after(activated, (down_term, lse)), w_down, (((1,), (0,)), ((), ())))
    d_gate_up = feed_back(after(d_branch, branch), w_down, gate_up)
    branch_own = branch[:own]
    branch = exchange_seq(
        [branch_own]
        + [branch[j * own : (j + 1) * own].astype(bf16) for j in range(1, n)], n)
    gate_up_term = pair_dot(h2_turned, d_gate_up, fs, 5)
    gate_up_grad = scatter_fsdp(gate_up_term, cores)
    (d_h2,) = dot_scatter(after(d_gate_up, gate_up_term), w_gate_up, n, 3)
    gain_two_grad = jnp.sum(d_h2 * normed_two, axis=0)
    bias_two_grad = jnp.sum(d_h2, axis=0)
    d_residual = d_own.astype(f32) + norm_back(d_h2, normed_two, inverse_two, gain_two)

    d_attended = d_residual.astype(bf16)
    d_mixed = jnp.concatenate(
        [dot(d_attended, item, across).astype(bf16) for item in w_out], axis=1
    )
    d_mixed = exchange(d_mixed, n, part, False, 2)
    d_projected = attend_back(
        slot, query, key, value, d_mixed, lse, tables
    )
    down_pieces = spread_seq(after(down_grad, d_mixed), n)
    qkv_term = pair_dot(h1_turned, d_projected, fs, 6)
    qkv_grad = scatter_fsdp(qkv_term, cores)
    d_h1, d_attended_part = dot_scatter(after(d_projected, qkv_term), w_first, n, 4, d_attended)
    mixed_all = jnp.concatenate([after(item, d_h1) for item in mixed_pieces], axis=0)
    out_term = dot(mixed_all, d_attended_part, down).astype(bf16)
    out_term = jnp.concatenate(by_core(out_term[:half], out_term[half:]), axis=0)
    d_h1_first, d_h1 = d_h1, after(d_h1, out_term)
    qkv_bias_part = jnp.sum(after(d_projected, d_h1).astype(f32), axis=0)
    gain_one_grad = jnp.sum(d_h1 * normed_one, axis=0)
    bias_one_grad = jnp.sum(d_h1, axis=0)

    branch = [branch_own] + [after(item, d_h1) for item in branch[1:]]
    block_out = (residual + sum(item.astype(f32) for item in branch)).astype(bf16)
    bias_all = jnp.concatenate(
        [jnp.where(s == i, qkv_bias_part.reshape(3, part), 0.0) for i in range(n)], axis=1
    )
    small = [
        gain_one_grad.reshape(fs, rows),
        bias_one_grad.reshape(fs, rows),
        gain_two_grad.reshape(fs, rows),
        bias_two_grad.reshape(fs, rows),
        bias_all.reshape(fs, 3 * rows),
    ]
    extra = -(-7 * rows // part)
    extra += -extra % 16
    small.append(jnp.zeros((fs, extra * part - 7 * rows), f32))
    small = jnp.concatenate(small, axis=1).astype(bf16).reshape(fs, extra, part)
    out_term = jnp.concatenate([out_term.reshape(fs, rows, part), small], axis=1)
    out_term = out_term.reshape(fs * (rows + extra), part)
    out_term = pair_sum(out_term)
    out_grad = scatter_fsdp(out_term, cores)
    input_grad = (
        d_residual + norm_back(after(d_h1, out_term), normed_one, inverse_one, gain_one)
    ).astype(bf16)

    down_total = jnp.stack(natural(down_pieces)).reshape(shard, width).astype(f32)
    gate_up_pieces = gather_streams(after(gate_up_grad, d_projected), n, d_h1_first)
    gate_total, up_total = finish(
        s, gate_up_pieces, (ffn, ffn),
        functools.partial(place_units, fs), min(64, rows // 2))
    qkv_pieces = gather_streams(after(qkv_grad, d_h1_first), n)
    (qkv_total,) = finish(
        s, qkv_pieces, (3 * width,),
        functools.partial(place_columns, 3), min(64, rows // 2))
    out_pieces = spread_seq(out_grad, n)
    (out_total,) = finish(
        s, [out_pieces], (width,),
        functools.partial(place_columns, 1), rows, rows)
    sums = sum(got[rows:].astype(f32) for got in out_pieces).reshape(extra * part)
    return (
        block_out[None],
        input_grad[None],
        sums[:rows],
        sums[rows : 2 * rows],
        qkv_total,
        sums[4 * rows : 7 * rows],
        out_total,
        sums[2 * rows : 3 * rows],
        sums[3 * rows : 4 * rows],
        gate_total,
        up_total,
        down_total,
    )


def solution(mesh):
    split = P("fsdp", None)
    act = P("fsdp", "seq", None)
    vec = P("fsdp")
    return jax.shard_map(
        functools.partial(body, n=mesh.shape["seq"], fs=mesh.shape["fsdp"]),
        mesh=mesh,
        in_specs=(act, act, P(), vec, vec, split, vec, split, vec, vec, split, split, split),
        out_specs=(act, act, vec, vec, split, vec, split, vec, vec, split, split, split),
        check_vma=False,
    )
```
